256 devices in a mesh: col: 64 (over z, x, core), row: 4 (over y).
Axes of the slice: x: 4, y: 4, z: 8, core: 2. Of those that a mesh axis runs over, the one named last changes fastest.
Arguments:
- slab: float32 [1024, 262144], P('row', 'col'), may hold values from -6 to 6
- omega: float32 [262144, 256], P('col'), may hold values from -0.01171875 to 0.01171875
- y_prev: float32 [65536, 256], P(('row', 'col')), may hold values from -0.6 to 0.6
- w_prev: float32 [512, 262144], P('row', 'col'), may hold values from -6 to 6
- prev_bucket: int32 [65536], P(('row', 'col')), may hold values from 0 to 511
- prev_sign: int32 [65536], P(('row', 'col')), may hold values from 0 to 1
- slab_bucket: int32 [1024], P('row'), may hold values from 0 to 511
- slab_sign: int32 [1024], P('row'), may hold values from 0 to 1
Outputs:
- q_prev: float32 [65536, 256], P(('row', 'col'))
- q_slab: float32 [1024, 256], P(('row', 'col'))
- x_core: float32 [256, 262144], P('row', 'col')
The draws below stay inside these ranges and needn't reach their ends.
All inputs are finite; a program needn't handle non-finite values.
Results may differ from the reference program's by a relative error of at most 0.00016.
Values sent between devices are 32-bit elements; how exact they have to be, the bound alone decides.
A program may use at most 64 MiB of HBM per device.

```python
import jax
import jax.numpy as jnp
from jax import lax

K = 256
L = 512
N = 262144
SLAB = 1024
PREV = 65536


def touch_ends(drawn, key, low, largest):
    spot = [jax.random.randint(jax.random.fold_in(key, axis), (), 0, length) for axis, length in enumerate(drawn.shape)]
    longest = drawn.shape.index(max(drawn.shape))
    next_to = spot[:longest] + [(spot[longest] + 1) % drawn.shape[longest]] + spot[longest + 1:]
    return drawn.at[tuple(spot)].set(low).at[tuple(next_to)].set(largest)


def levels(key, dims, cuts, smallest, largest):
    loudness, own = 1.0, jax.random.fold_in(key, 6)
    for dim, blocks in cuts:
        draws = jnp.exp(jax.random.uniform(jax.random.fold_in(own, dim), (blocks,), jnp.float32, smallest / len(cuts), largest / len(cuts)))
        loudness = loudness * jnp.repeat(draws, dims[dim] // blocks).reshape([-1 if axis == dim else 1 for axis in range(len(dims))])
    return loudness


def noise(own_key, shape, deviation, reach, split=(), dtype=jnp.bfloat16):
    factor_of = levels(own_key, shape, split, -0.22, 0.18) if split else 1.0
    values = jax.random.normal(own_key, shape, jnp.float32) * deviation * factor_of
    return jnp.minimum(jnp.maximum(values, -reach), reach).astype(dtype)


def setup_inputs(seed: int = 0) -> dict:
    arg_keys = jax.random.split(jax.random.key(seed), 9)
    return {
        "slab": noise(arg_keys[0], (SLAB, N), 1.0, 6.0, ((0, 4), (1, 64)), jnp.float32),
        "omega": noise(arg_keys[1], (N, K), N ** -0.5, 0.01171875, ((0, 64),), jnp.float32),
        "y_prev": noise(arg_keys[2], (PREV, K), 0.1, 0.6, ((0, 256),), jnp.float32),
        "w_prev": noise(arg_keys[3], (L, N), 1.0, 6.0, ((0, 4), (1, 64)), jnp.float32),
        "prev_bucket": touch_ends(jax.random.randint(arg_keys[4], (PREV,), 0, L), jax.random.fold_in(arg_keys[4], 1), 0, L - 1).astype(jnp.int32),
        "prev_sign": touch_ends(jax.random.randint(arg_keys[5], (PREV,), 0, 2), jax.random.fold_in(arg_keys[5], 1), 0, 1).astype(jnp.int32),
        "slab_bucket": touch_ends(jax.random.randint(arg_keys[6], (SLAB,), 0, L), jax.random.fold_in(arg_keys[6], 1), 0, L - 1).astype(jnp.int32),
        "slab_sign": touch_ends(jax.random.randint(arg_keys[7], (SLAB,), 0, 2), jax.random.fold_in(arg_keys[7], 1), 0, 1).astype(jnp.int32),
    }


def reference(slab, omega, y_prev, w_prev, prev_bucket, prev_sign, slab_bucket, slab_sign):
    highest = lax.Precision.HIGHEST
    y_slab = jnp.dot(slab.astype(jnp.float32), omega.astype(jnp.float32), precision=highest, preferred_element_type=jnp.float32)
    y_all = jnp.concatenate([y_prev, y_slab], axis=0)
    gram = jnp.dot(y_all.T.astype(jnp.float32), y_all.astype(jnp.float32), precision=highest, preferred_element_type=jnp.float32)
    lower = jnp.linalg.cholesky(gram)
    q_all = jax.scipy.linalg.solve_triangular(lower, y_all.T, lower=True).T
    buckets = jnp.concatenate([prev_bucket, slab_bucket]).astype(jnp.int32)
    signs = (2 * jnp.concatenate([prev_sign, slab_sign]) - 1).astype(jnp.float32)
    sketched = jax.ops.segment_sum(q_all * signs[:, None], buckets, num_segments=L)
    slab_signs = (2 * slab_sign - 1).astype(jnp.float32)
    w_new = w_prev + jax.ops.segment_sum(slab * slab_signs[:, None], slab_bucket.astype(jnp.int32), num_segments=L)
    curv = jnp.dot(sketched.T.astype(jnp.float32), sketched.astype(jnp.float32), precision=highest, preferred_element_type=jnp.float32)
    curv_lower = jnp.linalg.cholesky(curv)
    mapping = jax.scipy.linalg.cho_solve((curv_lower, True), sketched.T)
    x_core = jnp.dot(mapping.astype(jnp.float32), w_new.astype(jnp.float32), precision=highest, preferred_element_type=jnp.float32)
    return (q_all[:PREV], q_all[PREV:], x_core)
```

```python
import jax
import jax.numpy as jnp
from jax import lax
from jax.experimental import pallas as pl
from jax.experimental.pallas import tpu as pltpu
from jax.sharding import Mesh
from jax.sharding import PartitionSpec as P

L = 512
COL = ("col_0", "col_1", "col_2")
ROW_COL = ("row", "col_0", "col_1", "col_2")


highest = lax.Precision.HIGHEST


def in_blocks(x, dim, size):
    before, after = (x.shape[:dim], x.shape[dim + 1 :])
    return jnp.moveaxis(x.reshape(*before, size, -1, *after), dim, 0)


def sum_at_owner(x, axis, dim):
    size = lax.axis_size(axis)
    blocks = lax.all_to_all(in_blocks(x, dim, size), axis, 0, 0, tiled=True)
    return jnp.sum(blocks, axis=0)


def sum_in_two_steps(x, axes, dim):
    far, near = axes
    blocks = in_blocks(x, dim, lax.axis_size(far))
    nearer = sum_at_owner(blocks, near, dim + 1)
    arrived = lax.all_to_all(nearer, far, split_axis=0, concat_axis=0, tiled=True)
    return arrived.sum(axis=0)


def filled_up(lines, size):
    spare = -lines.shape[0] % size
    if not spare:
        return lines
    return jnp.concatenate([lines, jnp.zeros((spare, *lines.shape[1:]), lines.dtype)])


def from_everyone(x, axis):
    copies = jnp.broadcast_to(x, (lax.axis_size(axis), *x.shape))
    return lax.all_to_all(copies, axis, split_axis=0, concat_axis=0, tiled=True)


def in_order(blocks, dim):
    shape = list(blocks.shape[1:])
    shape[dim] *= blocks.shape[0]
    return jnp.moveaxis(blocks, 0, dim).reshape(shape)


def gathered_by_axis(x, axes, dim):
    far, near = axes
    blocks = from_everyone(from_everyone(x, far), near)
    return in_order(blocks.swapaxes(0, 1).reshape(-1, *x.shape), dim)


def sum_by_parts(x, axes):
    lines = x.reshape(-1, x.shape[-1])
    own = sum_in_two_steps(
        filled_up(lines, lax.axis_size(axes[0]) * lax.axis_size(axes[1])), axes, 0
    )
    whole = gathered_by_axis(own, axes, 0)
    return whole[: len(lines)].reshape(x.shape)


def matmul(left, right):
    return jnp.dot(left, right, precision=highest, preferred_element_type=jnp.float32)


def signed_table(bucket, sign, height):
    levels = lax.broadcasted_iota(jnp.int32, (height, bucket.shape[0]), 0)
    signs = (2 * sign - 1).astype(jnp.float32)
    return jnp.where(levels == bucket[None, :], signs[None, :], 0.0)


K = 256
BLK = 16
SUP = 64


def mm(a, b, dims=((1,), (0,))):
    return lax.dot_general(a, b, (dims, ((), ())), precision=highest, preferred_element_type=jnp.float32)


def eliminate(panel, k):
    off = k * BLK
    tile = off // 128 * 128
    cols = []
    for j in range(BLK):
        c = off + j
        cols.append([jnp.broadcast_to(panel[h * 8 : h * 8 + 8, c : c + 1], (8, 128)) for h in (0, 1)])
    lane = lax.broadcasted_iota(jnp.int32, (8, K), 1)
    row = lax.broadcasted_iota(jnp.int32, (8, K), 0)
    row1 = lax.broadcasted_iota(jnp.int32, (8, 128), 0)
    inside = (lane >= off) & (lane < off + BLK)
    top = jnp.where(inside, (lane == row + off).astype(jnp.float32), panel[:8])
    bot = jnp.where(inside, (lane == row + off + 8).astype(jnp.float32), panel[8:])
    lane1 = lax.broadcasted_iota(jnp.int32, (8, 128), 1) + tile
    corner = [jnp.zeros((8, 128), jnp.float32), jnp.zeros((8, 128), jnp.float32)]
    scales = []
    for j in range(BLK):
        h, r = divmod(j, 8)
        mine = cols[j]
        pivot = jnp.broadcast_to(mine[h][r : r + 1], (8, 128))
        rs = lax.rsqrt(pivot)
        inv = rs * rs
        scales.append(rs)
        low = mine[1] * inv
        high = None
        if h == 0:
            high = mine[0] * inv
        for m in range(j + 1, BLK):
            hm, rm = divmod(m, 8)
            u = jnp.broadcast_to(mine[hm][rm : rm + 1], (8, 128))
            cols[m][1] = cols[m][1] - low * u
            if hm == 0:
                cols[m][0] = cols[m][0] - high * u
        if h == 0:
            p = jnp.broadcast_to(top[r : r + 1], (8, K))
            hm_ = jnp.where(row1 > r, high, 0.0)
            top = top - jnp.concatenate([hm_, hm_], axis=1) * p
            bot = bot - jnp.concatenate([low, low], axis=1) * p
        else:
            p = jnp.broadcast_to(bot[r : r + 1], (8, K))
            lm_ = jnp.where(row1 > r, low, 0.0)
            bot = bot - jnp.concatenate([lm_, lm_], axis=1) * p
    st = jnp.zeros((8, 128), jnp.float32)
    sb = jnp.zeros((8, 128), jnp.float32)
    for j in range(8):
        st = jnp.where(row1 == j, scales[j], st)
        sb = jnp.where(row1 == j, scales[j + 8], sb)
    top = top * jnp.concatenate([st, st], axis=1)
    bot = bot * jnp.concatenate([sb, sb], axis=1)
    for j in range(BLK):
        for h in (0, 1):
            keep = (lane1 == off + j) & (row1 + 8 * h >= j)
            corner[h] = jnp.where(keep, cols[j][h] * scales[j], corner[h])
    return jnp.concatenate([top, bot], axis=0), jnp.concatenate(corner, axis=0)


def factor_step(w, u, k):
    off = k * BLK
    rows = slice(off, off + BLK)
    panel, corner = eliminate(w[rows, :], k)
    tile = off // 128 * 128
    w[rows, :] = panel
    lane = lax.broadcasted_iota(jnp.int32, (BLK, K), 1)
    upper = jnp.where(lane >= off + BLK, panel, 0.0)
    u[rows, :] = upper
    sup_end = (off // SUP + 1) * SUP
    if off + BLK < sup_end:
        turned = panel[:, tile : tile + 128].T
        left = turned[off + BLK - tile : sup_end - tile]
        rest = slice(off + BLK, sup_end)
        lane2 = lax.broadcasted_iota(jnp.int32, (sup_end - off - BLK, K), 1)
        old = jnp.where((lane2 >= off) & (lane2 < off + BLK), 0.0, w[rest, :])
        w[rest, :] = old - mm(left, panel)
    elif sup_end < K:
        start = sup_end - SUP
        block = w[start:sup_end, :]
        t0 = sup_end // 128 * 128
        turned = block[:, t0:].T
        left = turned[sup_end - t0 :]
        rest = slice(sup_end, K)
        lane2 = lax.broadcasted_iota(jnp.int32, (K - sup_end, K), 1)
        old = jnp.where((lane2 >= start) & (lane2 < sup_end), 0.0, w[rest, :])
        lane3 = lax.broadcasted_iota(jnp.int32, (SUP, K), 1)
        row3 = lax.broadcasted_iota(jnp.int32, (SUP, K), 0) + start
        block = jnp.where((lane3 < sup_end) & (lane3 > row3), 0.0, block)
        w[rest, :] = old - mm(left, block)
    return corner


def factor_both(wg, ws, ug, us):
    for k in range(K // BLK):
        cg = factor_step(wg, ug, k)
        factor_step(ws, us, k)
        off = k * BLK
        tile = off // 128 * 128
        rows = slice(off, off + BLK)
        turned = cg.T[off - tile : off - tile + BLK]
        ug[rows, off:off + BLK] = turned


def factors_kernel(gram, sketch, xg, mapping, u, xs, us):
    xg[...] = gram[...]
    xs[...] = mm(sketch[...], sketch[...], ((0,), (0,)))
    factor_both(xg, xs, u, us)
    row = lax.broadcasted_iota(jnp.int32, (K, K), 0)
    lane = lax.broadcasted_iota(jnp.int32, (K, K), 1)
    xg[...] = jnp.where(lane <= row, xg[...], 0.0)
    inner = jnp.where(lane <= row, xs[...], 0.0)
    core = mm(mm(u[...], inner, ((1,), (1,))), inner)
    mapping[...] = mm(core, sketch[...], ((1,), (1,)))


def factors(gram, sketch):
    vmem = pl.BlockSpec(memory_space=pltpu.VMEM)
    return pl.pallas_call(
        factors_kernel,
        out_shape=(
            jax.ShapeDtypeStruct((K, K), jnp.float32),
            jax.ShapeDtypeStruct((K, L), jnp.float32),
        ),
        in_specs=[vmem] * 2,
        out_specs=[vmem] * 2,
        scratch_shapes=[pltpu.VMEM((K, K), jnp.float32)] * 3,
        cost_estimate=pl.CostEstimate(flops=12_000_000_000, bytes_accessed=2_000_000, transcendentals=0),
        name="factors",
    )(gram, sketch)


def on_device(slab, omega, y_prev, w_prev, prev_bucket, prev_sign, slab_bucket, slab_sign):
    col_count = lax.axis_size(COL)
    col_place = lax.axis_index(COL)
    row_place = lax.axis_index("row")
    share = slab.shape[0] // col_count
    y_new = sum_in_two_steps(matmul(slab, omega), (("col_0", "col_1"), "col_2"), 0)
    leaf = jnp.concatenate([y_prev, y_new], axis=0)
    own_bucket = jnp.concatenate(
        [prev_bucket, lax.dynamic_slice_in_dim(slab_bucket, col_place * share, share, 0)]
    )
    own_sign = jnp.concatenate(
        [prev_sign, lax.dynamic_slice_in_dim(slab_sign, col_place * share, share, 0)]
    )
    local_table = signed_table(own_bucket, own_sign, L)
    both = jnp.concatenate([matmul(local_table, leaf), matmul(leaf.T, leaf)], axis=0)
    both = sum_by_parts(both, (("col_0", "col_1"), ("col_2", "row")))
    inverse, mapping = factors(both[L:], both[:L])
    q_leaf = matmul(leaf, inverse.T)
    lshare = w_prev.shape[0]
    own_cols = lax.dynamic_slice_in_dim(mapping, row_place * lshare, lshare, 1)
    slab_table = signed_table(slab_bucket, slab_sign, L)
    combined = matmul(mapping, slab_table)
    first = matmul(combined, slab)
    x_core = sum_at_owner(first + matmul(own_cols, w_prev), "row", 0)
    return (q_leaf[: y_prev.shape[0]], q_leaf[y_prev.shape[0] :], x_core)


def solution(mesh):
    finer = Mesh(
        mesh.devices.reshape(8, 4, 2, mesh.shape["row"]), ("col_0", "col_1", "col_2", "row")
    )
    return jax.shard_map(
        on_device,
        mesh=finer,
        in_specs=(
            P("row", COL),
            P(COL, None),
            P(ROW_COL, None),
            P("row", COL),
            P(ROW_COL),
            P(ROW_COL),
            P("row"),
            P("row"),
        ),
        out_specs=(P(ROW_COL, None), P(ROW_COL, None), P("row", COL)),
        check_vma=False,
    )
```

```python
import functools

import jax
import jax.numpy as jnp
from jax import lax
from jax.experimental import pallas as pl
from jax.experimental.pallas import tpu as pltpu
from jax.sharding import Mesh
from jax.sharding import PartitionSpec as P

L = 512
COL = ("z", "x", "core")
ROW_COL = ("y", "z", "x", "core")
MESH = pl.DeviceIdType.MESH
highest = lax.Precision.HIGHEST
K = 256
BLK = 16
SUP = 64


def mm(a, b, dims=((1,), (0,))):
    return lax.dot_general(a, b, (dims, ((), ())), precision=highest, preferred_element_type=jnp.float32)


def eliminate(panel, k):
    off = k * BLK
    tile = off // 128 * 128
    cols = []
    for j in range(BLK):
        c = off + j
        cols.append([jnp.broadcast_to(panel[h * 8 : h * 8 + 8, c : c + 1], (8, 128)) for h in (0, 1)])
    lane = lax.broadcasted_iota(jnp.int32, (8, K), 1)
    row = lax.broadcasted_iota(jnp.int32, (8, K), 0)
    row1 = lax.broadcasted_iota(jnp.int32, (8, 128), 0)
    inside = (lane >= off) & (lane < off + BLK)
    top = jnp.where(inside, (lane == row + off).astype(jnp.float32), panel[:8])
    bot = jnp.where(inside, (lane == row + off + 8).astype(jnp.float32), panel[8:])
    lane1 = lax.broadcasted_iota(jnp.int32, (8, 128), 1) + tile
    corner = [jnp.zeros((8, 128), jnp.float32), jnp.zeros((8, 128), jnp.float32)]
    scales = []
    for j in range(BLK):
        h, r = divmod(j, 8)
        mine = cols[j]
        pivot = jnp.broadcast_to(mine[h][r : r + 1], (8, 128))
        rs = lax.rsqrt(pivot)
        inv = rs * rs
        scales.append(rs)
        low = mine[1] * inv
        high = None
        if h == 0:
            high = mine[0] * inv
        for m in range(j + 1, BLK):
            hm, rm = divmod(m, 8)
            u = jnp.broadcast_to(mine[hm][rm : rm + 1], (8, 128))
            cols[m][1] = cols[m][1] - low * u
            if hm == 0:
                cols[m][0] = cols[m][0] - high * u
        if h == 0:
            p = jnp.broadcast_to(top[r : r + 1], (8, K))
            hm_ = jnp.where(row1 > r, high, 0.0)
            top = top - jnp.concatenate([hm_, hm_], axis=1) * p
            bot = bot - jnp.concatenate([low, low], axis=1) * p
        else:
            p = jnp.broadcast_to(bot[r : r + 1], (8, K))
            lm_ = jnp.where(row1 > r, low, 0.0)
            bot = bot - jnp.concatenate([lm_, lm_], axis=1) * p
    st = jnp.zeros((8, 128), jnp.float32)
    sb = jnp.zeros((8, 128), jnp.float32)
    for j in range(8):
        st = jnp.where(row1 == j, scales[j], st)
        sb = jnp.where(row1 == j, scales[j + 8], sb)
    top = top * jnp.concatenate([st, st], axis=1)
    bot = bot * jnp.concatenate([sb, sb], axis=1)
    for j in range(BLK):
        for h in (0, 1):
            keep = (lane1 == off + j) & (row1 + 8 * h >= j)
            corner[h] = jnp.where(keep, cols[j][h] * scales[j], corner[h])
    return jnp.concatenate([top, bot], axis=0), jnp.concatenate(corner, axis=0)


def factor_step(w, u, k):
    off = k * BLK
    rows = slice(off, off + BLK)
    panel, corner = eliminate(w[rows, :], k)
    tile = off // 128 * 128
    w[rows, :] = panel
    lane = lax.broadcasted_iota(jnp.int32, (BLK, K), 1)
    upper = jnp.where(lane >= off + BLK, panel, 0.0)
    u[rows, :] = upper
    sup_end = (off // SUP + 1) * SUP
    if off + BLK < sup_end:
        turned = panel[:, tile : tile + 128].T
        left = turned[off + BLK - tile : sup_end - tile]
        rest = slice(off + BLK, sup_end)
        lane2 = lax.broadcasted_iota(jnp.int32, (sup_end - off - BLK, K), 1)
        old = jnp.where((lane2 >= off) & (lane2 < off + BLK), 0.0, w[rest, :])
        w[rest, :] = old - mm(left, panel)
    elif sup_end < K:
        start = sup_end - SUP
        block = w[start:sup_end, :]
        t0 = sup_end // 128 * 128
        turned = block[:, t0:].T
        left = turned[sup_end - t0 :]
        rest = slice(sup_end, K)
        lane2 = lax.broadcasted_iota(jnp.int32, (K - sup_end, K), 1)
        old = jnp.where((lane2 >= start) & (lane2 < sup_end), 0.0, w[rest, :])
        lane3 = lax.broadcasted_iota(jnp.int32, (SUP, K), 1)
        row3 = lax.broadcasted_iota(jnp.int32, (SUP, K), 0) + start
        block = jnp.where((lane3 < sup_end) & (lane3 > row3), 0.0, block)
        w[rest, :] = old - mm(left, block)
    return corner


def factor_both(wg, ws, ug, us):
    for k in range(K // BLK):
        cg = factor_step(wg, ug, k)
        factor_step(ws, us, k)
        off = k * BLK
        tile = off // 128 * 128
        rows = slice(off, off + BLK)
        turned = cg.T[off - tile : off - tile + BLK]
        ug[rows, off:off + BLK] = turned


NZ, NX, NC, NY = 8, 4, 2, 4
CHUNK = 512
SUMS = L + K
PART_A = SUMS // NY
PART_B = PART_A // NX
PIECE = K // NX
BLOCK = PIECE + PART_B + 8


def split(v):
    high = v.astype(jnp.bfloat16)
    return high, (v - high.astype(jnp.float32)).astype(jnp.bfloat16)


def mul(a, b, dims=((1,), (0,))):
    return lax.dot_general(a, b, (dims, ((), ())), preferred_element_type=jnp.float32)


def mul3(a, b, dims=((1,), (0,))):
    ah, al = split(a)
    bh, bl = split(b)
    return mul(ah, bh, dims) + (mul(ah, bl, dims) + mul(al, bh, dims))


def signed_sum(table, v):
    high = v.astype(jnp.bfloat16)
    rest = v - high.astype(jnp.float32)
    mid = rest.astype(jnp.bfloat16)
    low = (rest - mid.astype(jnp.float32)).astype(jnp.bfloat16)
    return mul(table, high) + (mul(table, mid) + mul(table, low))


def table_of(bucket, sign):
    level = lax.broadcasted_iota(jnp.int32, (L, bucket.shape[1]), 0).astype(jnp.float32)
    return jnp.where(level == bucket, 2.0 * sign - 1.0, 0.0).astype(jnp.bfloat16)


def sums_kernel(slab, omega, y_prev, prev_bs, slab_bs, out, slab_v, omega_v, stack, part, got_a, got_b, got_s,
                got_c, got_z, mid_p, mid_a, mid_s, load_sem, a_sem, b_sem, s_sem, c_sem, z_sem, d_sem, e_sem, f_sem, g_sem):
    z, x, c, y = (lax.axis_index(name) for name in ("z", "x", "core", "y"))

    def at(dz=0, dx=0, dc=0, dy=0):
        return {"z": (z + dz) % NZ, "x": (x + dx) % NX, "core": (c + dc) % NC, "y": (y + dy) % NY}

    def send(src, dst, sems, i, where):
        copy = pltpu.make_async_remote_copy(
            src_ref=src, dst_ref=dst, send_sem=sems.at[0, i], recv_sem=sems.at[1, i], device_id=where, device_id_type=MESH
        )
        copy.start()
        return copy

    barrier = pltpu.get_barrier_semaphore()
    peers = [at(dz=d) for d in range(1, NZ)]
    peers += [at(dy=d, dc=e) for d in range(NY) for e in range(NC) if d or e]
    peers += [at(dx=d, dc=e) for d in range(1, NX) for e in range(NC)]
    for peer in peers:
        pl.semaphore_signal(barrier, inc=1, device_id=peer, device_id_type=MESH)

    chunks = slab_v.shape[0]
    loads = []
    for i in range(chunks):
        loads.append(pltpu.make_async_copy(slab.at[:, pl.ds(i * CHUNK, CHUNK)], slab_v.at[i], load_sem.at[0, i]))
        loads.append(pltpu.make_async_copy(omega.at[pl.ds(i * CHUNK, CHUNK), :], omega_v.at[i], load_sem.at[1, i]))
    for load in loads:
        load.start()

    table = jnp.concatenate([table_of(prev_bs[h : h + 1, :], prev_bs[h + 2 : h + 3, :]) for h in (0, 1)], axis=1)
    own = y_prev[...]
    stack[:L, :] = signed_sum(table, own)
    stack[L:, :] = mm(own, own, ((0,), (0,)))
    out[c, y, x, PIECE + PART_B :, :] = slab_bs[...]

    pl.semaphore_wait(barrier, len(peers))

    group = [(d, e) for d in range(NY) for e in range(NC) if d or e]
    sent_a = []
    for i, (d, e) in enumerate(group):
        where = at(dy=d, dc=e)
        piece = stack.at[pl.ds(pl.multiple_of(where["y"] * PART_A, 8), PART_A), pl.ds(pl.multiple_of(where["core"] * 128, 128), 128)]
        sent_a.append(send(piece, got_a.at[i], a_sem, i, where))

    part[...] = jnp.zeros_like(part)

    @pl.loop(0, chunks)
    def _(i):
        pltpu.make_async_copy(slab.at[:, pl.ds(0, CHUNK)], slab_v.at[i], load_sem.at[0, i]).wait()
        pltpu.make_async_copy(omega.at[pl.ds(0, CHUNK), :], omega_v.at[i], load_sem.at[1, i]).wait()
        part[...] += mul3(slab_v[i], omega_v[i])

    sent_b = []
    for i, (d, e) in enumerate(group):
        where = at(dx=d, dc=e)
        piece = part.at[pl.ds(pl.multiple_of(where["x"] * PIECE, 8), PIECE), pl.ds(pl.multiple_of(where["core"] * 128, 128), 128)]
        sent_b.append(send(piece, got_b.at[i], b_sem, i, where))

    for copy in sent_a:
        copy.wait_recv()
    total = stack[pl.ds(pl.multiple_of(y * PART_A, 8), PART_A), pl.ds(pl.multiple_of(c * 128, 128), 128)]
    for i in range(len(group)):
        total = total + got_a[i]
    mid_a[...] = total
    sent_s = []
    for d in range(1, NX):
        where = at(dx=d)
        piece = mid_a.at[pl.ds(pl.multiple_of(where["x"] * PART_B, 8), PART_B), :]
        sent_s.append(send(piece, got_s.at[d - 1], s_sem, d - 1, where))

    for copy in sent_b:
        copy.wait_recv()
    total = part[pl.ds(pl.multiple_of(x * PIECE, 8), PIECE), pl.ds(pl.multiple_of(c * 128, 128), 128)]
    for i in range(len(group)):
        total = total + got_b[i]
    mid_p[...] = total
    sent_c = []
    for d in range(1, NZ):
        where = at(dz=d)
        piece = mid_p.at[pl.ds(pl.multiple_of(where["z"] * 8, 8), 8), :]
        sent_c.append(send(piece, got_c.at[d - 1], c_sem, d - 1, where))

    for copy in sent_s:
        copy.wait_recv()
    total = mid_a[pl.ds(pl.multiple_of(x * PART_B, 8), PART_B), :]
    for d in range(1, NX):
        total = total + got_s[d - 1]
    mid_s[...] = total
    sent_z = [send(mid_s, got_z.at[d - 1], z_sem, d - 1, at(dz=d)) for d in range(1, NZ)]

    for copy in sent_c:
        copy.wait_recv()
    total = mid_p[pl.ds(pl.multiple_of(z * 8, 8), 8), :]
    for d in range(1, NZ):
        total = total + got_c[d - 1]
    tile = pl.ds(pl.multiple_of(z * 8, 8), 8)
    out[c, y, x, tile, :] = total
    sent_d = [send(out.at[c, y, x, tile, :], out.at[c, y, x, tile, :], d_sem, d - 1, at(dz=d)) for d in range(1, NZ)]

    for copy in sent_z:
        copy.wait_recv()
    total = mid_s[...]
    for d in range(1, NZ):
        total = total + got_z[d - 1]
    out[c, y, x, PIECE : PIECE + PART_B, :] = total
    for copy in sent_d:
        copy.wait_recv()

    def first(d):
        return at(dx=d * (1 - c), dy=d * c)

    def second(d):
        return at(dx=d * c, dy=d * (1 - c))

    def spread(block, n, along_first):
        copies = []
        if along_first:
            copies += [send(block, block, e_sem, d - 1, first(d)) for d in range(1, 4)]
        if n < 4:
            copies += [send(block, block, f_sem, 3 * n + d - 1, second(d)) for d in range(1, 4)]
        copies.append(send(block, block, g_sem, n, at(dc=1)))
        return copies

    own_block = out.at[c, y, x]
    sent = spread(own_block, 0, True)
    sent_e, sent_f, sent_g = sent[:3], sent[3:6], sent[6:]
    for d in range(1, 4):
        sent_e[d - 1].wait_recv()
        block = out.at[c, (y + (4 - d) * c) % NY, (x + (4 - d) * (1 - c)) % NX]
        more = spread(block, d, False)
        sent_f += more[:3]
        sent_g += more[3:]
    for n in range(4):
        for d in range(1, 4):
            sent_f[3 * n + d - 1].wait_recv()
            by = (y + (4 - n) * c + (4 - d) * (1 - c)) % NY
            bx = (x + (4 - n) * (1 - c) + (4 - d) * c) % NX
            sent_g += spread(out.at[c, by, bx], 4 + 3 * n + d - 1, False)
    for copy in sent_g:
        copy.wait_recv()
    for copy in sent_a + sent_b + sent_s + sent_c + sent_z + sent_d + sent_e + sent_f + sent_g:
        copy.wait_send()


def sums(slab, omega, y_prev, prev_bs, slab_bs):
    rows, cols = slab.shape
    chunks = cols // CHUNK
    vmem = pl.BlockSpec(memory_space=pltpu.VMEM)
    hbm = pl.BlockSpec(memory_space=pl.ANY)
    f32 = jnp.float32
    dma = pltpu.SemaphoreType.DMA
    return pl.pallas_call(
        sums_kernel,
        out_shape=jax.ShapeDtypeStruct((NC, NY, NX, BLOCK, 128), f32),
        in_specs=[hbm, hbm, vmem, vmem, vmem],
        out_specs=vmem,
        scratch_shapes=[
            pltpu.VMEM((chunks, rows, CHUNK), f32),
            pltpu.VMEM((chunks, CHUNK, K), f32),
            pltpu.VMEM((SUMS, K), f32),
            pltpu.VMEM((rows, K), f32),
            pltpu.VMEM((7, PART_A, 128), f32),
            pltpu.VMEM((7, PIECE, 128), f32),
            pltpu.VMEM((3, PART_B, 128), f32),
            pltpu.VMEM((7, 8, 128), f32),
            pltpu.VMEM((7, PART_B, 128), f32),
            pltpu.VMEM((PIECE, 128), f32),
            pltpu.VMEM((PART_A, 128), f32),
            pltpu.VMEM((PART_B, 128), f32),
            dma((2, chunks)),
            dma((2, 7)),
            dma((2, 7)),
            dma((2, 3)),
            dma((2, 7)),
            dma((2, 7)),
            dma((2, 7)),
            dma((2, 3)),
            dma((2, 12)),
            dma((2, 16)),
        ],
        compiler_params=pltpu.CompilerParams(collective_id=0, has_side_effects=True, vmem_limit_bytes=40 * 2**20),
        cost_estimate=pl.CostEstimate(flops=60_000_000_000, bytes_accessed=10_000_000, transcendentals=0),
        name="sums",
    )(slab, omega, y_prev, prev_bs, slab_bs)


def factors_kernel(place, gathered, y_prev, q_prev, q_new, combined, xg, xs, u, us, ys, zs, ts, mapping):
    for c in range(NC):
        lanes = slice(128 * c, 128 * c + 128)
        for y in range(NY):
            for x in range(NX):
                ys[pl.ds(256 * y + PIECE * x, PIECE), lanes] = gathered[c, y, x, :PIECE, :]
                zs[pl.ds(PART_A * y + PART_B * x, PART_B), lanes] = gathered[c, y, x, PIECE : PIECE + PART_B, :]
    for y in range(NY):
        bs = gathered[0, y, 0, PIECE + PART_B :, :]
        for h in (0, 1):
            ts[:, 256 * y + 128 * h : 256 * y + 128 * h + 128] = table_of(bs[h : h + 1], bs[h + 2 : h + 3])
    new = ys[...]
    xg[...] = zs[L:, :] + mm(new, new, ((0,), (0,)))
    zs[:L, :] = zs[:L, :] + signed_sum(ts[...], new)
    sketch = zs[:L, :]
    xs[...] = mm(sketch, sketch, ((0,), (0,)))
    factor_both(xg, xs, u, us)
    row = lax.broadcasted_iota(jnp.int32, (K, K), 0)
    lane = lax.broadcasted_iota(jnp.int32, (K, K), 1)
    outer = jnp.where(lane <= row, xg[...], 0.0)
    inner = jnp.where(lane <= row, xs[...], 0.0)
    core = mm(mm(u[...], inner, ((1,), (1,))), inner)
    found = mm(core, zs[:L, :], ((1,), (1,)))
    mapping[...] = found
    y_place = place[0]
    cols = pl.ds(pl.multiple_of(y_place * 256, 256), 256)
    table = ts[:, cols]
    high = found.astype(jnp.bfloat16)
    rest = found - high.astype(jnp.float32)
    mid = rest.astype(jnp.bfloat16)
    low = (rest - mid.astype(jnp.float32)).astype(jnp.bfloat16)
    combined[:, :256] = mul(high, table) + (mul(mid, table) + mul(low, table))
    combined[:, 256:] = mapping[:, pl.ds(pl.multiple_of(y_place * 128, 128), 128)]
    q_prev[...] = mm(y_prev[...], outer, ((1,), (1,)))
    q_new[...] = mm(ys[pl.ds(pl.multiple_of(place[1] * 8, 8), 8), :], outer, ((1,), (1,)))


def factors(place, gathered, y_prev):
    vmem = pl.BlockSpec(memory_space=pltpu.VMEM)
    f32 = jnp.float32
    return pl.pallas_call(
        factors_kernel,
        out_shape=(
            jax.ShapeDtypeStruct(y_prev.shape, f32),
            jax.ShapeDtypeStruct((8, K), f32),
            jax.ShapeDtypeStruct((K, 384), f32),
        ),
        in_specs=[pl.BlockSpec(memory_space=pltpu.SMEM), vmem, vmem],
        out_specs=[vmem] * 3,
        scratch_shapes=[pltpu.VMEM((K, K), f32)] * 4
        + [pltpu.VMEM((1024, K), f32), pltpu.VMEM((SUMS, K), f32), pltpu.VMEM((L, 1024), jnp.bfloat16), pltpu.VMEM((K, L), f32)],
        compiler_params=pltpu.CompilerParams(vmem_limit_bytes=40 * 2**20),
        cost_estimate=pl.CostEstimate(flops=20_000_000_000, bytes_accessed=3_000_000, transcendentals=0),
        name="factors",
    )(place, gathered, y_prev)


def in_blocks(x, dim, size):
    before, after = (x.shape[:dim], x.shape[dim + 1 :])
    return jnp.moveaxis(x.reshape(*before, size, -1, *after), dim, 0)


def sum_at_owner(x, axis, dim):
    size = lax.axis_size(axis)
    blocks = lax.all_to_all(in_blocks(x, dim, size), axis, 0, 0, tiled=True)
    return jnp.sum(blocks, axis=0)


def matmul(left, right):
    return jnp.dot(left, right, precision=highest, preferred_element_type=jnp.float32)


def as_rows(bucket, sign):
    rows = jnp.concatenate([bucket.reshape(2, 128), sign.reshape(2, 128)]).astype(jnp.float32)
    return jnp.concatenate([rows, jnp.zeros((4, 128), jnp.float32)])


def on_device(slab, omega, y_prev, w_prev, prev_bucket, prev_sign, slab_bucket, slab_sign):
    y = lax.axis_index("y")
    col = lax.axis_index(COL)
    gathered = sums(slab, omega, y_prev, as_rows(prev_bucket, prev_sign), as_rows(slab_bucket, slab_sign))
    place = jnp.stack([y, y * 32 + col // 2]).astype(jnp.int32)
    q_prev, q_pair, combined = factors(place, gathered, y_prev)
    q_new = lax.dynamic_slice_in_dim(q_pair, (col % 2) * 4, 4, 0)
    first = matmul(combined[:, :256], slab)
    x_core = sum_at_owner(first + matmul(combined[:, 256:], w_prev), "y", 0)
    return (q_prev, q_new, x_core)


def solution(mesh):
    finer = Mesh(mesh.devices.reshape(NZ, NX, NC, NY), ("z", "x", "core", "y"))
    return jax.shard_map(
        on_device,
        mesh=finer,
        in_specs=(
            P("y", COL),
            P(COL, None),
            P(ROW_COL, None),
            P("y", COL),
            P(ROW_COL),
            P(ROW_COL),
            P("y"),
            P("y"),
        ),
        out_specs=(P(ROW_COL, None), P(ROW_COL, None), P("y", COL)),
        check_vma=False,
    )
```

```python
import jax
import jax.numpy as jnp
from jax import lax
from jax.experimental import pallas as pl
from jax.experimental.pallas import tpu as pltpu
from jax.sharding import Mesh
from jax.sharding import PartitionSpec as P

L = 512
COL = ("z", "x", "core")
ROW_COL = ("y", "z", "x", "core")
MESH = pl.DeviceIdType.MESH
highest = lax.Precision.HIGHEST
K = 256
BLK = 16
SUP = 64


def mm(a, b, dims=((1,), (0,))):
    return lax.dot_general(a, b, (dims, ((), ())), precision=highest, preferred_element_type=jnp.float32)


def eliminate(panel, k):
    off = k * BLK
    tile = off // 128 * 128
    cols = []
    for j in range(BLK):
        c = off + j
        cols.append([jnp.broadcast_to(panel[h * 8 : h * 8 + 8, c : c + 1], (8, 128)) for h in (0, 1)])
    lane = lax.broadcasted_iota(jnp.int32, (8, K), 1)
    row = lax.broadcasted_iota(jnp.int32, (8, K), 0)
    row1 = lax.broadcasted_iota(jnp.int32, (8, 128), 0)
    inside = (lane >= off) & (lane < off + BLK)
    top = jnp.where(inside, (lane == row + off).astype(jnp.float32), panel[:8])
    bot = jnp.where(inside, (lane == row + off + 8).astype(jnp.float32), panel[8:])
    lane1 = lax.broadcasted_iota(jnp.int32, (8, 128), 1) + tile
    corner = [jnp.zeros((8, 128), jnp.float32), jnp.zeros((8, 128), jnp.float32)]
    scales = []
    for j in range(BLK):
        h, r = divmod(j, 8)
        mine = cols[j]
        pivot = jnp.broadcast_to(mine[h][r : r + 1], (8, 128))
        rs = lax.rsqrt(pivot)
        inv = rs * rs
        scales.append(rs)
        low = mine[1] * inv
        high = None
        if h == 0:
            high = mine[0] * inv
        for m in range(j + 1, BLK):
            hm, rm = divmod(m, 8)
            u = jnp.broadcast_to(mine[hm][rm : rm + 1], (8, 128))
            cols[m][1] = cols[m][1] - low * u
            if hm == 0:
                cols[m][0] = cols[m][0] - high * u
        if h == 0:
            p = jnp.broadcast_to(top[r : r + 1], (8, K))
            hm_ = jnp.where(row1 > r, high, 0.0)
            top = top - jnp.concatenate([hm_, hm_], axis=1) * p
            bot = bot - jnp.concatenate([low, low], axis=1) * p
        else:
            p = jnp.broadcast_to(bot[r : r + 1], (8, K))
            lm_ = jnp.where(row1 > r, low, 0.0)
            bot = bot - jnp.concatenate([lm_, lm_], axis=1) * p
    st = jnp.zeros((8, 128), jnp.float32)
    sb = jnp.zeros((8, 128), jnp.float32)
    for j in range(8):
        st = jnp.where(row1 == j, scales[j], st)
        sb = jnp.where(row1 == j, scales[j + 8], sb)
    top = top * jnp.concatenate([st, st], axis=1)
    bot = bot * jnp.concatenate([sb, sb], axis=1)
    for j in range(BLK):
        for h in (0, 1):
            keep = (lane1 == off + j) & (row1 + 8 * h >= j)
            corner[h] = jnp.where(keep, cols[j][h] * scales[j], corner[h])
    return jnp.concatenate([top, bot], axis=0), jnp.concatenate(corner, axis=0)


def factor_step(w, u, k):
    off = k * BLK
    rows = slice(off, off + BLK)
    panel, corner = eliminate(w[rows, :], k)
    tile = off // 128 * 128
    w[rows, :] = panel
    lane = lax.broadcasted_iota(jnp.int32, (BLK, K), 1)
    upper = jnp.where(lane >= off + BLK, panel, 0.0)
    u[rows, :] = upper
    sup_end = (off // SUP + 1) * SUP
    if off + BLK < sup_end:
        turned = panel[:, tile : tile + 128].T
        left = turned[off + BLK - tile : sup_end - tile]
        rest = slice(off + BLK, sup_end)
        lane2 = lax.broadcasted_iota(jnp.int32, (sup_end - off - BLK, K), 1)
        old = jnp.where((lane2 >= off) & (lane2 < off + BLK), 0.0, w[rest, :])
        w[rest, :] = old - mm(left, panel)
    elif sup_end < K:
        start = sup_end - SUP
        block = w[start:sup_end, :]
        t0 = sup_end // 128 * 128
        turned = block[:, t0:].T
        left = turned[sup_end - t0 :]
        rest = slice(sup_end, K)
        lane2 = lax.broadcasted_iota(jnp.int32, (K - sup_end, K), 1)
        old = jnp.where((lane2 >= start) & (lane2 < sup_end), 0.0, w[rest, :])
        lane3 = lax.broadcasted_iota(jnp.int32, (SUP, K), 1)
        row3 = lax.broadcasted_iota(jnp.int32, (SUP, K), 0) + start
        block = jnp.where((lane3 < sup_end) & (lane3 > row3), 0.0, block)
        w[rest, :] = old - mm(left, block)
    return corner


def factor_both(wg, ws, ug, us):
    for k in range(K // BLK):
        cg = factor_step(wg, ug, k)
        factor_step(ws, us, k)
        off = k * BLK
        tile = off // 128 * 128
        rows = slice(off, off + BLK)
        turned = cg.T[off - tile : off - tile + BLK]
        ug[rows, off:off + BLK] = turned


NZ, NX, NC, NY = 8, 4, 2, 4
CHUNK = 512
SUMS = L + K
PART_A = SUMS // NY
PART_B = PART_A // NX
PIECE = K // NX
BLOCK = PIECE + PART_B + 8


def split(v):
    high = v.astype(jnp.bfloat16)
    return high, (v - high.astype(jnp.float32)).astype(jnp.bfloat16)


def mul(a, b, dims=((1,), (0,))):
    return lax.dot_general(a, b, (dims, ((), ())), preferred_element_type=jnp.float32)


def mul3(a, b, dims=((1,), (0,))):
    ah, al = split(a)
    bh, bl = split(b)
    return mul(ah, bh, dims) + (mul(ah, bl, dims) + mul(al, bh, dims))


def signed_sum(table, v):
    high = v.astype(jnp.bfloat16)
    rest = v - high.astype(jnp.float32)
    mid = rest.astype(jnp.bfloat16)
    low = (rest - mid.astype(jnp.float32)).astype(jnp.bfloat16)
    return mul(table, high) + (mul(table, mid) + mul(table, low))


def table_of(bucket, sign):
    level = lax.broadcasted_iota(jnp.int32, (L, bucket.shape[1]), 0).astype(jnp.float32)
    return jnp.where(level == bucket, 2.0 * sign - 1.0, 0.0).astype(jnp.bfloat16)


def sums_kernel(slab, omega, y_prev, prev_bs, slab_bs, out, slab_v, omega_v, stack, part, got_a, got_b, got_s,
                got_c, got_z, mid_p, mid_a, mid_s, load_sem, a_sem, b_sem, s_sem, c_sem, z_sem, d_sem, e_sem, f_sem, g_sem):
    z, x, c, y = (lax.axis_index(name) for name in ("z", "x", "core", "y"))

    def at(dz=0, dx=0, dc=0, dy=0):
        return {"z": (z + dz) % NZ, "x": (x + dx) % NX, "core": (c + dc) % NC, "y": (y + dy) % NY}

    def send(src, dst, sems, i, where):
        copy = pltpu.make_async_remote_copy(
            src_ref=src, dst_ref=dst, send_sem=sems.at[0, i], recv_sem=sems.at[1, i], device_id=where, device_id_type=MESH
        )
        copy.start()
        return copy

    barrier = pltpu.get_barrier_semaphore()
    peers = [at(dz=d) for d in range(1, NZ)]
    peers += [at(dy=d, dc=e) for d in range(NY) for e in range(NC) if d or e]
    peers += [at(dx=d, dc=e) for d in range(1, NX) for e in range(NC)]
    for peer in peers:
        pl.semaphore_signal(barrier, inc=1, device_id=peer, device_id_type=MESH)

    chunks = slab_v.shape[0]
    loads = []
    for i in range(chunks):
        loads.append(pltpu.make_async_copy(slab.at[:, pl.ds(i * CHUNK, CHUNK)], slab_v.at[i], load_sem.at[0, i]))
        loads.append(pltpu.make_async_copy(omega.at[pl.ds(i * CHUNK, CHUNK), :], omega_v.at[i], load_sem.at[1, i]))
    for load in loads:
        load.start()

    table = jnp.concatenate([table_of(prev_bs[h : h + 1, :], prev_bs[h + 2 : h + 3, :]) for h in (0, 1)], axis=1)
    own = y_prev[...]
    stack[:L, :] = signed_sum(table, own)
    stack[L:, :] = mm(own, own, ((0,), (0,)))
    out[c, y, x, PIECE + PART_B :, :] = slab_bs[...]

    pl.semaphore_wait(barrier, len(peers))

    group = [(d, e) for d in range(NY) for e in range(NC) if d or e]
    sent_a = []
    for i, (d, e) in enumerate(group):
        where = at(dy=d, dc=e)
        piece = stack.at[pl.ds(pl.multiple_of(where["y"] * PART_A, 8), PART_A), pl.ds(pl.multiple_of(where["core"] * 128, 128), 128)]
        sent_a.append(send(piece, got_a.at[i], a_sem, i, where))

    part[...] = jnp.zeros_like(part)

    @pl.loop(0, chunks)
    def _(i):
        pltpu.make_async_copy(slab.at[:, pl.ds(0, CHUNK)], slab_v.at[i], load_sem.at[0, i]).wait()
        pltpu.make_async_copy(omega.at[pl.ds(0, CHUNK), :], omega_v.at[i], load_sem.at[1, i]).wait()
        part[...] += mul3(slab_v[i], omega_v[i])

    sent_b = []
    for i, (d, e) in enumerate(group):
        where = at(dx=d, dc=e)
        piece = part.at[pl.ds(pl.multiple_of(where["x"] * PIECE, 8), PIECE), pl.ds(pl.multiple_of(where["core"] * 128, 128), 128)]
        sent_b.append(send(piece, got_b.at[i], b_sem, i, where))

    for copy in sent_a:
        copy.wait_recv()
    total = stack[pl.ds(pl.multiple_of(y * PART_A, 8), PART_A), pl.ds(pl.multiple_of(c * 128, 128), 128)]
    for i in range(len(group)):
        total = total + got_a[i]
    mid_a[...] = total
    sent_s = []
    for d in range(1, NX):
        where = at(dx=d)
        piece = mid_a.at[pl.ds(pl.multiple_of(where["x"] * PART_B, 8), PART_B), :]
        sent_s.append(send(piece, got_s.at[d - 1], s_sem, d - 1, where))

    for copy in sent_b:
        copy.wait_recv()
    total = part[pl.ds(pl.multiple_of(x * PIECE, 8), PIECE), pl.ds(pl.multiple_of(c * 128, 128), 128)]
    for i in range(len(group)):
        total = total + got_b[i]
    mid_p[...] = total
    sent_c = []
    for d in range(1, NZ):
        where = at(dz=d)
        piece = mid_p.at[pl.ds(pl.multiple_of(where["z"] * 8, 8), 8), :]
        sent_c.append(send(piece, got_c.at[d - 1], c_sem, d - 1, where))

    for copy in sent_s:
        copy.wait_recv()
    total = mid_a[pl.ds(pl.multiple_of(x * PART_B, 8), PART_B), :]
    for d in range(1, NX):
        total = total + got_s[d - 1]
    mid_s[...] = total
    sent_z = [send(mid_s, got_z.at[d - 1], z_sem, d - 1, at(dz=d)) for d in range(1, NZ)]

    for copy in sent_c:
        copy.wait_recv()
    total = mid_p[pl.ds(pl.multiple_of(z * 8, 8), 8), :]
    for d in range(1, NZ):
        total = total + got_c[d - 1]
    tile = pl.ds(pl.multiple_of(z * 8, 8), 8)
    out[c, y, x, tile, :] = total
    sent_d = [send(out.at[c, y, x, tile, :], out.at[c, y, x, tile, :], d_sem, d - 1, at(dz=d)) for d in range(1, NZ)]

    for copy in sent_z:
        copy.wait_recv()
    total = mid_s[...]
    for d in range(1, NZ):
        total = total + got_z[d - 1]
    out[c, y, x, PIECE : PIECE + PART_B, :] = total
    for copy in sent_d:
        copy.wait_recv()

    def first(d):
        return at(dx=d * (1 - c), dy=d * c)

    def second(d):
        return at(dx=d * c, dy=d * (1 - c))

    def spread(block, n, along_first):
        copies = []
        if along_first:
            copies += [send(block, block, e_sem, d - 1, first(d)) for d in range(1, 4)]
        if n < 4:
            copies += [send(block, block, f_sem, 3 * n + d - 1, second(d)) for d in range(1, 4)]
        copies.append(send(block, block, g_sem, n, at(dc=1)))
        return copies

    own_block = out.at[c, y, x]
    sent = spread(own_block, 0, True)
    sent_e, sent_f, sent_g = sent[:3], sent[3:6], sent[6:]
    for d in range(1, 4):
        sent_e[d - 1].wait_recv()
        block = out.at[c, (y + (4 - d) * c) % NY, (x + (4 - d) * (1 - c)) % NX]
        more = spread(block, d, False)
        sent_f += more[:3]
        sent_g += more[3:]
    for n in range(4):
        for d in range(1, 4):
            sent_f[3 * n + d - 1].wait_recv()
            by = (y + (4 - n) * c + (4 - d) * (1 - c)) % NY
            bx = (x + (4 - n) * (1 - c) + (4 - d) * c) % NX
            sent_g += spread(out.at[c, by, bx], 4 + 3 * n + d - 1, False)
    for copy in sent_g:
        copy.wait_recv()
    for copy in sent_a + sent_b + sent_s + sent_c + sent_z + sent_d + sent_e + sent_f + sent_g:
        copy.wait_send()


def sums(slab, omega, y_prev, prev_bs, slab_bs):
    rows, cols = slab.shape
    chunks = cols // CHUNK
    vmem = pl.BlockSpec(memory_space=pltpu.VMEM)
    hbm = pl.BlockSpec(memory_space=pltpu.HBM)
    f32 = jnp.float32
    dma = pltpu.SemaphoreType.DMA
    return pl.pallas_call(
        sums_kernel,
        out_shape=jax.ShapeDtypeStruct((NC, NY, NX, BLOCK, 128), f32),
        in_specs=[hbm, hbm, vmem, vmem, vmem],
        out_specs=vmem,
        scratch_shapes=[
            pltpu.VMEM((chunks, rows, CHUNK), f32),
            pltpu.VMEM((chunks, CHUNK, K), f32),
            pltpu.VMEM((SUMS, K), f32),
            pltpu.VMEM((rows, K), f32),
            pltpu.VMEM((7, PART_A, 128), f32),
            pltpu.VMEM((7, PIECE, 128), f32),
            pltpu.VMEM((3, PART_B, 128), f32),
            pltpu.VMEM((7, 8, 128), f32),
            pltpu.VMEM((7, PART_B, 128), f32),
            pltpu.VMEM((PIECE, 128), f32),
            pltpu.VMEM((PART_A, 128), f32),
            pltpu.VMEM((PART_B, 128), f32),
            dma((2, chunks)),
            dma((2, 7)),
            dma((2, 7)),
            dma((2, 3)),
            dma((2, 7)),
            dma((2, 7)),
            dma((2, 7)),
            dma((2, 3)),
            dma((2, 12)),
            dma((2, 16)),
        ],
        compiler_params=pltpu.CompilerParams(collective_id=0, has_side_effects=True, vmem_limit_bytes=63_500_000),
        cost_estimate=pl.CostEstimate(flops=60_000_000_000, bytes_accessed=10_000_000, transcendentals=0),
        name="sums",
    )(slab, omega, y_prev, prev_bs, slab_bs)


def factors_kernel(place, gathered, y_prev, q_prev, q_new, combined, xg, xs, u, us, ys, zs, ts, mapping):
    for c in range(NC):
        lanes = slice(128 * c, 128 * c + 128)
        for y in range(NY):
            for x in range(NX):
                ys[pl.ds(256 * y + PIECE * x, PIECE), lanes] = gathered[c, y, x, :PIECE, :]
                zs[pl.ds(PART_A * y + PART_B * x, PART_B), lanes] = gathered[c, y, x, PIECE : PIECE + PART_B, :]
    for y in range(NY):
        bs = gathered[0, y, 0, PIECE + PART_B :, :]
        for h in (0, 1):
            ts[:, 256 * y + 128 * h : 256 * y + 128 * h + 128] = table_of(bs[h : h + 1], bs[h + 2 : h + 3])
    new = ys[...]
    xg[...] = zs[L:, :] + mm(new, new, ((0,), (0,)))
    zs[:L, :] = zs[:L, :] + signed_sum(ts[...], new)
    sketch = zs[:L, :]
    xs[...] = mm(sketch, sketch, ((0,), (0,)))
    factor_both(xg, xs, u, us)
    row = lax.broadcasted_iota(jnp.int32, (K, K), 0)
    lane = lax.broadcasted_iota(jnp.int32, (K, K), 1)
    outer = jnp.where(lane <= row, xg[...], 0.0)
    inner = jnp.where(lane <= row, xs[...], 0.0)
    core = mm(mm(u[...], inner, ((1,), (1,))), inner)
    found = mm(core, zs[:L, :], ((1,), (1,)))
    mapping[...] = found
    y_place = place[0]
    cols = pl.ds(pl.multiple_of(y_place * 256, 256), 256)
    table = ts[:, cols]
    high = found.astype(jnp.bfloat16)
    rest = found - high.astype(jnp.float32)
    mid = rest.astype(jnp.bfloat16)
    low = (rest - mid.astype(jnp.float32)).astype(jnp.bfloat16)
    combined[:, :256] = mul(high, table) + (mul(mid, table) + mul(low, table))
    combined[:, 256:] = mapping[:, pl.ds(pl.multiple_of(y_place * 128, 128), 128)]
    q_prev[...] = mm(y_prev[...], outer, ((1,), (1,)))
    q_new[...] = mm(ys[pl.ds(pl.multiple_of(place[1] * 8, 8), 8), :], outer, ((1,), (1,)))


def factors(place, gathered, y_prev):
    vmem = pl.BlockSpec(memory_space=pltpu.VMEM)
    f32 = jnp.float32
    return pl.pallas_call(
        factors_kernel,
        out_shape=(
            jax.ShapeDtypeStruct(y_prev.shape, f32),
            jax.ShapeDtypeStruct((8, K), f32),
            jax.ShapeDtypeStruct((K, 384), f32),
        ),
        in_specs=[pl.BlockSpec(memory_space=pltpu.SMEM), vmem, vmem],
        out_specs=[vmem] * 3,
        scratch_shapes=[pltpu.VMEM((K, K), f32)] * 4
        + [pltpu.VMEM((1024, K), f32), pltpu.VMEM((SUMS, K), f32), pltpu.VMEM((L, 1024), jnp.bfloat16), pltpu.VMEM((K, L), f32)],
        compiler_params=pltpu.CompilerParams(vmem_limit_bytes=40 * 2**20),
        cost_estimate=pl.CostEstimate(flops=20_000_000_000, bytes_accessed=3_000_000, transcendentals=0),
        name="factors",
    )(place, gathered, y_prev)


def core_kernel(combined, slab, w_prev, out, terms, far_l, far_r, near_l, near_r, far_sem, near_sem):
    y = lax.axis_index("y")
    chunks = terms.shape[0]
    half = chunks // 2
    rows = out.shape[0]
    up, down, across = (y + 1) % NY, (y + 3) % NY, (y + 2) % NY

    barrier = pltpu.get_barrier_semaphore()
    for peer in (up, down):
        pl.semaphore_signal(barrier, inc=1, device_id={"y": peer}, device_id_type=MESH)
    order = [n for i in range(half) for n in (i, half + i)]

    def block(n, place):
        return terms.at[n, pl.ds(pl.multiple_of(place * rows, 8), rows), :]

    def send(src, dst, send_sem, recv_sem, peer):
        return pltpu.make_async_remote_copy(
            src_ref=src, dst_ref=dst, send_sem=send_sem, recv_sem=recv_sem, device_id={"y": peer}, device_id_type=MESH
        )

    far = [
        send(block(n, across), far_l.at[n], far_sem.at[0, n], far_sem.at[1, n], up)
        if n < half
        else send(block(n, across), far_r.at[n - half], far_sem.at[0, n], far_sem.at[1, n], down)
        for n in range(chunks)
    ]
    to_up = [send(block(n, up), near_l.at[n], near_sem.at[0, n], near_sem.at[1, n], up) for n in range(chunks)]
    to_down = [send(block(n, down), near_r.at[n], near_sem.at[2, n], near_sem.at[3, n], down) for n in range(chunks)]

    for i, n in enumerate(order):
        cols = slice(n * CHUNK, n * CHUNK + CHUNK)
        terms[n] = mul3(combined[...], jnp.concatenate([slab[:, cols], w_prev[:, cols]], axis=0))
        if i == 0:
            pl.semaphore_wait(barrier, 2)
        far[n].start()
    for i in range(half):
        to_up[half + i].start()
        to_down[i].start()
    for i in range(half):
        far[i].wait_recv()
        spot = pl.ds(pl.multiple_of(up * rows, 8), rows)
        terms[i, spot, :] = terms[i, spot, :] + far_l[i]
        to_up[i].start()
        far[half + i].wait_recv()
        spot = pl.ds(pl.multiple_of(down * rows, 8), rows)
        terms[half + i, spot, :] = terms[half + i, spot, :] + far_r[i]
        to_down[half + i].start()
    own = pl.ds(pl.multiple_of(y * rows, 8), rows)
    for i in range(half):
        for n in (i, half + i):
            to_up[n].wait_recv()
            to_down[n].wait_recv()
            out[:, n * CHUNK : n * CHUNK + CHUNK] = terms[n, own, :] + (near_l[n] + near_r[n])
    for copy in far + to_up + to_down:
        copy.wait_send()


def core_product(combined, slab, w_prev):
    cols = slab.shape[1]
    chunks = cols // CHUNK
    rows = K // NY
    vmem = pl.BlockSpec(memory_space=pltpu.VMEM)
    f32 = jnp.float32
    dma = pltpu.SemaphoreType.DMA
    return pl.pallas_call(
        core_kernel,
        out_shape=jax.ShapeDtypeStruct((rows, cols), f32),
        in_specs=[vmem, vmem, vmem],
        out_specs=vmem,
        scratch_shapes=[
            pltpu.VMEM((chunks, K, CHUNK), f32),
            pltpu.VMEM((chunks // 2, rows, CHUNK), f32),
            pltpu.VMEM((chunks // 2, rows, CHUNK), f32),
            pltpu.VMEM((chunks, rows, CHUNK), f32),
            pltpu.VMEM((chunks, rows, CHUNK), f32),
            dma((2, chunks)),
            dma((4, chunks)),
        ],
        compiler_params=pltpu.CompilerParams(collective_id=1, has_side_effects=True, vmem_limit_bytes=40 * 2**20),
        cost_estimate=pl.CostEstimate(flops=60_000_000_000, bytes_accessed=10_000_000, transcendentals=0),
        name="core_product",
    )(combined, slab, w_prev)


def as_rows(bucket, sign):
    rows = jnp.concatenate([bucket.reshape(2, 128), sign.reshape(2, 128)]).astype(jnp.float32)
    return jnp.concatenate([rows, jnp.zeros((4, 128), jnp.float32)])


def on_device(slab, omega, y_prev, w_prev, prev_bucket, prev_sign, slab_bucket, slab_sign):
    y = lax.axis_index("y")
    col = lax.axis_index(COL)
    gathered = sums(slab, omega, y_prev, as_rows(prev_bucket, prev_sign), as_rows(slab_bucket, slab_sign))
    place = jnp.stack([y, y * 32 + col // 2]).astype(jnp.int32)
    q_prev, q_pair, combined = factors(place, gathered, y_prev)
    q_new = lax.dynamic_slice_in_dim(q_pair, (col % 2) * 4, 4, 0)
    x_core = core_product(combined, slab, w_prev)
    return (q_prev, q_new, x_core)


def solution(mesh):
    finer = Mesh(mesh.devices.reshape(NZ, NX, NC, NY), ("z", "x", "core", "y"))
    return jax.shard_map(
        on_device,
        mesh=finer,
        in_specs=(
            P("y", COL),
            P(COL, None),
            P(ROW_COL, None),
            P("y", COL),
            P(ROW_COL),
            P(ROW_COL),
            P("y"),
            P("y"),
        ),
        out_specs=(P(ROW_COL, None), P(ROW_COL, None), P("y", COL)),
        check_vma=False,
    )
```

```python
import jax
import jax.numpy as jnp
from jax import lax
from jax.experimental import pallas as pl
from jax.experimental.pallas import tpu as pltpu
from jax.sharding import Mesh
from jax.sharding import PartitionSpec as P

L = 512
COL = ("z", "x", "core")
ROW_COL = ("y", "z", "x", "core")
MESH = pl.DeviceIdType.MESH
highest = lax.Precision.HIGHEST
K = 256
BLK = 16
SUP = 64


def mm(a, b, dims=((1,), (0,))):
    return lax.dot_general(a, b, (dims, ((), ())), precision=highest, preferred_element_type=jnp.float32)


def eliminate(panel, k):
    off = k * BLK
    tile = off // 128 * 128
    cols = []
    for j in range(BLK):
        c = off + j
        cols.append([jnp.broadcast_to(panel[h * 8 : h * 8 + 8, c : c + 1], (8, 128)) for h in (0, 1)])
    lane = lax.broadcasted_iota(jnp.int32, (8, K), 1)
    row = lax.broadcasted_iota(jnp.int32, (8, K), 0)
    row1 = lax.broadcasted_iota(jnp.int32, (8, 128), 0)
    inside = (lane >= off) & (lane < off + BLK)
    top = jnp.where(inside, (lane == row + off).astype(jnp.float32), panel[:8])
    bot = jnp.where(inside, (lane == row + off + 8).astype(jnp.float32), panel[8:])
    lane1 = lax.broadcasted_iota(jnp.int32, (8, 128), 1) + tile
    corner = [jnp.zeros((8, 128), jnp.float32), jnp.zeros((8, 128), jnp.float32)]
    scales = []
    for j in range(BLK):
        h, r = divmod(j, 8)
        mine = cols[j]
        pivot = jnp.broadcast_to(mine[h][r : r + 1], (8, 128))
        rs = lax.rsqrt(pivot)
        inv = rs * rs
        scales.append(rs)
        low = mine[1] * inv
        high = None
        if h == 0:
            high = mine[0] * inv
        for m in range(j + 1, BLK):
            hm, rm = divmod(m, 8)
            u = jnp.broadcast_to(mine[hm][rm : rm + 1], (8, 128))
            cols[m][1] = cols[m][1] - low * u
            if hm == 0:
                cols[m][0] = cols[m][0] - high * u
        if h == 0:
            p = jnp.broadcast_to(top[r : r + 1], (8, K))
            hm_ = jnp.where(row1 > r, high, 0.0)
            top = top - jnp.concatenate([hm_, hm_], axis=1) * p
            bot = bot - jnp.concatenate([low, low], axis=1) * p
        else:
            p = jnp.broadcast_to(bot[r : r + 1], (8, K))
            lm_ = jnp.where(row1 > r, low, 0.0)
            bot = bot - jnp.concatenate([lm_, lm_], axis=1) * p
    st = jnp.zeros((8, 128), jnp.float32)
    sb = jnp.zeros((8, 128), jnp.float32)
    for j in range(8):
        st = jnp.where(row1 == j, scales[j], st)
        sb = jnp.where(row1 == j, scales[j + 8], sb)
    top = top * jnp.concatenate([st, st], axis=1)
    bot = bot * jnp.concatenate([sb, sb], axis=1)
    for j in range(BLK):
        for h in (0, 1):
            keep = (lane1 == off + j) & (row1 + 8 * h >= j)
            corner[h] = jnp.where(keep, cols[j][h] * scales[j], corner[h])
    return jnp.concatenate([top, bot], axis=0), jnp.concatenate(corner, axis=0)


def factor_step(w, u, k):
    off = k * BLK
    rows = slice(off, off + BLK)
    panel, corner = eliminate(w[rows, :], k)
    tile = off // 128 * 128
    w[rows, :] = panel
    lane = lax.broadcasted_iota(jnp.int32, (BLK, K), 1)
    upper = jnp.where(lane >= off + BLK, panel, 0.0)
    u[rows, :] = upper
    sup_end = (off // SUP + 1) * SUP
    if off + BLK < sup_end:
        turned = panel[:, tile : tile + 128].T
        left = turned[off + BLK - tile : sup_end - tile]
        rest = slice(off + BLK, sup_end)
        lane2 = lax.broadcasted_iota(jnp.int32, (sup_end - off - BLK, K), 1)
        old = jnp.where((lane2 >= off) & (lane2 < off + BLK), 0.0, w[rest, :])
        w[rest, :] = old - mm(left, panel)
    elif sup_end < K:
        start = sup_end - SUP
        block = w[start:sup_end, :]
        t0 = sup_end // 128 * 128
        turned = block[:, t0:].T
        left = turned[sup_end - t0 :]
        rest = slice(sup_end, K)
        lane2 = lax.broadcasted_iota(jnp.int32, (K - sup_end, K), 1)
        old = jnp.where((lane2 >= start) & (lane2 < sup_end), 0.0, w[rest, :])
        lane3 = lax.broadcasted_iota(jnp.int32, (SUP, K), 1)
        row3 = lax.broadcasted_iota(jnp.int32, (SUP, K), 0) + start
        block = jnp.where((lane3 < sup_end) & (lane3 > row3), 0.0, block)
        w[rest, :] = old - mm(left, block)
    return corner


def factor_both(wg, ws, ug, us):
    for k in range(K // BLK):
        cg = factor_step(wg, ug, k)
        factor_step(ws, us, k)
        off = k * BLK
        tile = off // 128 * 128
        rows = slice(off, off + BLK)
        turned = cg.T[off - tile : off - tile + BLK]
        ug[rows, off:off + BLK] = turned


NZ, NX, NC, NY = 8, 4, 2, 4
CHUNK = 512
SUMS = L + K
PART_A = SUMS // 2 // NY
PART_B = PART_A // NX
PIECE = K // NX
BLOCK = PIECE + 2 * PART_B + 8


def split(v):
    high = v.astype(jnp.bfloat16)
    return high, (v - high.astype(jnp.float32)).astype(jnp.bfloat16)


def mul(a, b, dims=((1,), (0,))):
    return lax.dot_general(a, b, (dims, ((), ())), preferred_element_type=jnp.float32)


def mul3(a, b, dims=((1,), (0,))):
    ah, al = split(a)
    bh, bl = split(b)
    return mul(ah, bh, dims) + (mul(ah, bl, dims) + mul(al, bh, dims))


def signed_sum(table, v):
    high = v.astype(jnp.bfloat16)
    rest = v - high.astype(jnp.float32)
    mid = rest.astype(jnp.bfloat16)
    low = (rest - mid.astype(jnp.float32)).astype(jnp.bfloat16)
    return mul(table, high) + (mul(table, mid) + mul(table, low))


def table_of(bucket, sign):
    level = lax.broadcasted_iota(jnp.int32, (L, bucket.shape[1]), 0).astype(jnp.float32)
    return jnp.where(level == bucket, 2.0 * sign - 1.0, 0.0).astype(jnp.bfloat16)


def sums_kernel(slab, omega, y_prev, prev_bucket, prev_sign, slab_bucket, slab_sign, out, slab_v, omega_v, stack, part, got_a, got_b, got_s,
                got_c, got_z, mid_p, mid_a, mid_s, load_sem, a_sem, b_sem, s_sem, c_sem, z_sem, d_sem, e_sem, f_sem, g_sem):
    z, x, c, y = (lax.axis_index(name) for name in ("z", "x", "core", "y"))

    def at(dz=0, dx=0, dc=0, dy=0):
        return {"z": (z + dz) % NZ, "x": (x + dx) % NX, "core": (c + dc) % NC, "y": (y + dy) % NY}

    def send(src, dst, sems, i, where):
        copy = pltpu.make_async_remote_copy(
            src_ref=src, dst_ref=dst, send_sem=sems.at[0, i], recv_sem=sems.at[1, i], device_id=where, device_id_type=MESH
        )
        copy.start()
        return copy

    barrier = pltpu.get_barrier_semaphore()
    peers = [at(dz=d) for d in range(1, NZ)]
    peers += [at(dy=d, dc=e) for d in range(NY) for e in range(NC) if d or e]
    peers += [at(dx=d, dc=e) for d in range(1, NX) for e in range(NC)]
    for peer in peers:
        pl.semaphore_signal(barrier, inc=1, device_id=peer, device_id_type=MESH)

    chunks = slab_v.shape[0]
    loads = []
    for i in range(chunks):
        loads.append(pltpu.make_async_copy(slab.at[:, pl.ds(i * CHUNK, CHUNK)], slab_v.at[i], load_sem.at[0, i]))
        loads.append(pltpu.make_async_copy(omega.at[pl.ds(i * CHUNK, CHUNK), :], omega_v.at[i], load_sem.at[1, i]))
    for load in loads:
        load.start()

    def real(ref):
        return ref[...].astype(jnp.float32)

    bucket, sign = real(prev_bucket), real(prev_sign)
    table = jnp.concatenate([table_of(bucket[h : h + 1], sign[h : h + 1]) for h in (0, 1)], axis=1)
    own = y_prev[...]
    stack[:L, :] = signed_sum(table, own)
    stack[L:, :] = mm(own, own, ((0,), (0,)))
    out[c, y, x, PIECE + 2 * PART_B :, :] = jnp.concatenate([real(slab_bucket), real(slab_sign), jnp.zeros((4, 128), jnp.float32)])
    part[...] = jnp.zeros_like(part)

    def multiply(i):
        pltpu.make_async_copy(slab.at[:, pl.ds(0, CHUNK)], slab_v.at[i], load_sem.at[0, i]).wait()
        pltpu.make_async_copy(omega.at[pl.ds(0, CHUNK), :], omega_v.at[i], load_sem.at[1, i]).wait()
        part[...] += mul3(slab_v[i], omega_v[i])

    pl.loop(0, 2)(multiply)
    pl.semaphore_wait(barrier, len(peers))

    group = [(d, e) for d in range(NY) for e in range(NC) if d or e]

    def share(half, where):
        place = where["x"] if half else where["y"]
        return (
            pl.ds(pl.multiple_of(half * (SUMS // 2) + place * PART_A, 8), PART_A),
            pl.ds(pl.multiple_of(where["core"] * 128, 128), 128),
        )

    sent_a = []
    for i, (d, e) in enumerate(group):
        for half in (0, 1):
            where = at(dx=d, dc=e) if half else at(dy=d, dc=e)
            sent_a.append(send(stack.at[share(half, where)], got_a.at[half, i], a_sem, 2 * i + half, where))

    pl.loop(2, chunks)(multiply)

    sent_b = []
    for i, (d, e) in enumerate(group):
        where = at(dx=d, dc=e)
        piece = part.at[pl.ds(pl.multiple_of(where["x"] * PIECE, 8), PIECE), pl.ds(pl.multiple_of(where["core"] * 128, 128), 128)]
        sent_b.append(send(piece, got_b.at[i], b_sem, i, where))

    for copy in sent_a:
        copy.wait_recv()
    for half in (0, 1):
        total = stack[share(half, at())]
        for i in range(len(group)):
            total = total + got_a[half, i]
        mid_a[half] = total
    sent_s = []
    for d in range(1, NX):
        for half in (0, 1):
            where = at(dy=d) if half else at(dx=d)
            place = where["y"] if half else where["x"]
            piece = mid_a.at[half, pl.ds(pl.multiple_of(place * PART_B, 8), PART_B), :]
            sent_s.append(send(piece, got_s.at[half, d - 1], s_sem, 2 * (d - 1) + half, where))

    for copy in sent_b:
        copy.wait_recv()
    total = part[pl.ds(pl.multiple_of(x * PIECE, 8), PIECE), pl.ds(pl.multiple_of(c * 128, 128), 128)]
    for i in range(len(group)):
        total = total + got_b[i]
    mid_p[...] = total
    sent_c = []
    for d in range(1, NZ):
        where = at(dz=d)
        piece = mid_p.at[pl.ds(pl.multiple_of(where["z"] * 8, 8), 8), :]
        sent_c.append(send(piece, got_c.at[d - 1], c_sem, d - 1, where))

    for copy in sent_s:
        copy.wait_recv()
    for half in (0, 1):
        total = mid_a[half, pl.ds(pl.multiple_of((y if half else x) * PART_B, 8), PART_B), :]
        for d in range(1, NX):
            total = total + got_s[half, d - 1]
        mid_s[half * PART_B : half * PART_B + PART_B, :] = total
    sent_z = [send(mid_s, got_z.at[d - 1], z_sem, d - 1, at(dz=d)) for d in range(1, NZ)]

    for copy in sent_c:
        copy.wait_recv()
    total = mid_p[pl.ds(pl.multiple_of(z * 8, 8), 8), :]
    for d in range(1, NZ):
        total = total + got_c[d - 1]
    tile = pl.ds(pl.multiple_of(z * 8, 8), 8)
    out[c, y, x, tile, :] = total
    sent_d = [send(out.at[c, y, x, tile, :], out.at[c, y, x, tile, :], d_sem, d - 1, at(dz=d)) for d in range(1, NZ)]

    for copy in sent_z:
        copy.wait_recv()
    total = mid_s[...]
    for d in range(1, NZ):
        total = total + got_z[d - 1]
    out[c, y, x, PIECE : PIECE + 2 * PART_B, :] = total
    for copy in sent_d:
        copy.wait_recv()

    def first(d):
        return at(dx=d * (1 - c), dy=d * c)

    def second(d):
        return at(dx=d * c, dy=d * (1 - c))

    def gathered(n, d):
        return out.at[c, (y + (4 - n) * c + (4 - d) * (1 - c)) % NY, (x + (4 - n) * (1 - c) + (4 - d) * c) % NX]

    def swap(n, d):
        block = gathered(n, d)
        return send(block, block, g_sem, 4 * n + d, at(dc=1))

    def both_ways(n):
        block = gathered(n, 0)
        return [send(block, block, f_sem, 3 * n + d - 1, second(d)) for d in (1, 3)]

    own_block = gathered(0, 0)
    sent_e = [send(own_block, own_block, e_sem, d - 1, first(d)) for d in range(1, 4)]
    sent_f = {0: both_ways(0)}
    sent_g = [swap(0, 0)]
    for n in (1, 3, 2):
        sent_e[n - 1].wait_recv()
        sent_f[n] = both_ways(n)
        sent_g.append(swap(n, 0))
    passed = []
    for n in (0, 1, 3, 2):
        for d in (1, 3):
            sent_f[n][d // 2].wait_recv()
            block = gathered(n, d)
            if d == (1, 3)[n % 2]:
                passed.append((n, send(block, block, f_sem, 3 * n + 1, second(d))))
            sent_g.append(swap(n, d))
    for n, copy in passed:
        copy.wait_recv()
        sent_g.append(swap(n, 2))
    sent_f = [copy for n in range(4) for copy in sent_f[n]] + [copy for _, copy in passed]
    for copy in sent_g:
        copy.wait_recv()
    for copy in sent_a + sent_b + sent_s + sent_c + sent_z + sent_d + sent_e + sent_f + sent_g:
        copy.wait_send()


def sums(slab, omega, y_prev, *marks):
    rows, cols = slab.shape
    chunks = cols // CHUNK
    vmem = pl.BlockSpec(memory_space=pltpu.VMEM)
    hbm = pl.BlockSpec(memory_space=pltpu.HBM)
    f32 = jnp.float32
    dma = pltpu.SemaphoreType.DMA
    return pl.pallas_call(
        sums_kernel,
        out_shape=jax.ShapeDtypeStruct((NC, NY, NX, BLOCK, 128), f32),
        in_specs=[hbm, hbm] + [vmem] * 5,
        out_specs=vmem,
        scratch_shapes=[
            pltpu.VMEM((chunks, rows, CHUNK), f32),
            pltpu.VMEM((chunks, CHUNK, K), f32),
            pltpu.VMEM((SUMS, K), f32),
            pltpu.VMEM((rows, K), f32),
            pltpu.VMEM((2, 7, PART_A, 128), f32),
            pltpu.VMEM((7, PIECE, 128), f32),
            pltpu.VMEM((2, 3, PART_B, 128), f32),
            pltpu.VMEM((7, 8, 128), f32),
            pltpu.VMEM((7, 2 * PART_B, 128), f32),
            pltpu.VMEM((PIECE, 128), f32),
            pltpu.VMEM((2, PART_A, 128), f32),
            pltpu.VMEM((2 * PART_B, 128), f32),
            dma((2, chunks)),
            dma((2, 14)),
            dma((2, 7)),
            dma((2, 6)),
            dma((2, 7)),
            dma((2, 7)),
            dma((2, 7)),
            dma((2, 3)),
            dma((2, 12)),
            dma((2, 16)),
        ],
        compiler_params=pltpu.CompilerParams(collective_id=0, has_side_effects=True, vmem_limit_bytes=62_900_000),
        cost_estimate=pl.CostEstimate(flops=60_000_000_000, bytes_accessed=10_000_000, transcendentals=0),
        name="sums",
    )(slab, omega, y_prev, *(mark.reshape(2, 128) for mark in marks))


def factors_kernel(gathered, y_prev, q_prev, q_new, combined, xg, xs, u, us, ys, zs, ts, mapping):
    for c in range(NC):
        lanes = slice(128 * c, 128 * c + 128)
        for y in range(NY):
            for x in range(NX):
                ys[pl.ds(256 * y + PIECE * x, PIECE), lanes] = gathered[c, y, x, :PIECE, :]
                for half in (0, 1):
                    start = half * (SUMS // 2) + (PART_A * x + PART_B * y if half else PART_A * y + PART_B * x)
                    rows = gathered[c, y, x, PIECE + half * PART_B : PIECE + half * PART_B + PART_B, :]
                    zs[pl.ds(start, PART_B), lanes] = rows
    for y in range(NY):
        bs = gathered[0, y, 0, PIECE + 2 * PART_B :, :]
        for h in (0, 1):
            ts[:, 256 * y + 128 * h : 256 * y + 128 * h + 128] = table_of(bs[h : h + 1], bs[h + 2 : h + 3])
    new = ys[...]
    xg[...] = zs[L:, :] + mm(new, new, ((0,), (0,)))
    zs[:L, :] = zs[:L, :] + signed_sum(ts[...], new)
    sketch = zs[:L, :]
    xs[...] = mm(sketch, sketch, ((0,), (0,)))
    factor_both(xg, xs, u, us)
    row = lax.broadcasted_iota(jnp.int32, (K, K), 0)
    lane = lax.broadcasted_iota(jnp.int32, (K, K), 1)
    outer = jnp.where(lane <= row, xg[...], 0.0)
    inner = jnp.where(lane <= row, xs[...], 0.0)
    core = mm(mm(u[...], inner, ((1,), (1,))), inner)
    found = mm(core, zs[:L, :], ((1,), (1,)))
    mapping[...] = found
    y_place = lax.axis_index("y")
    col = lax.axis_index(COL)
    cols = pl.ds(pl.multiple_of(y_place * 256, 256), 256)
    table = ts[:, cols]
    high = found.astype(jnp.bfloat16)
    rest = found - high.astype(jnp.float32)
    mid = rest.astype(jnp.bfloat16)
    low = (rest - mid.astype(jnp.float32)).astype(jnp.bfloat16)
    combined[:, :256] = mul(high, table) + (mul(mid, table) + mul(low, table))
    combined[:, 256:] = mapping[:, pl.ds(pl.multiple_of(y_place * 128, 128), 128)]
    q_prev[...] = mm(y_prev[...], outer, ((1,), (1,)))
    pair = mm(ys[pl.ds(pl.multiple_of(y_place * 256 + (col // 2) * 8, 8), 8), :], outer, ((1,), (1,)))
    q_new[...] = jnp.where(col % 2 == 0, pair[:4], pair[4:])


def factors(gathered, y_prev):
    vmem = pl.BlockSpec(memory_space=pltpu.VMEM)
    f32 = jnp.float32
    return pl.pallas_call(
        factors_kernel,
        out_shape=(
            jax.ShapeDtypeStruct(y_prev.shape, f32),
            jax.ShapeDtypeStruct((4, K), f32),
            jax.ShapeDtypeStruct((K, 384), f32),
        ),
        in_specs=[vmem, vmem],
        out_specs=[vmem] * 3,
        scratch_shapes=[pltpu.VMEM((K, K), f32)] * 4
        + [pltpu.VMEM((1024, K), f32), pltpu.VMEM((SUMS, K), f32), pltpu.VMEM((L, 1024), jnp.bfloat16), pltpu.VMEM((K, L), f32)],
        compiler_params=pltpu.CompilerParams(vmem_limit_bytes=40 * 2**20),
        cost_estimate=pl.CostEstimate(flops=20_000_000_000, bytes_accessed=3_000_000, transcendentals=0),
        name="factors",
    )(gathered, y_prev)


def core_kernel(combined, slab, w_prev, out, terms, far_l, far_r, near_l, near_r, far_sem, near_sem):
    y = lax.axis_index("y")
    chunks = terms.shape[0]
    half = chunks // 2
    rows = out.shape[0]
    up, down, across = (y + 1) % NY, (y + 3) % NY, (y + 2) % NY

    barrier = pltpu.get_barrier_semaphore()
    for peer in (up, down):
        pl.semaphore_signal(barrier, inc=1, device_id={"y": peer}, device_id_type=MESH)
    order = [n for i in range(half) for n in (i, half + i)]

    def block(n, place):
        return terms.at[n, pl.ds(pl.multiple_of(place * rows, 8), rows), :]

    def send(src, dst, send_sem, recv_sem, peer):
        return pltpu.make_async_remote_copy(
            src_ref=src, dst_ref=dst, send_sem=send_sem, recv_sem=recv_sem, device_id={"y": peer}, device_id_type=MESH
        )

    far = [
        send(block(n, across), far_l.at[n], far_sem.at[0, n], far_sem.at[1, n], up)
        if n < half
        else send(block(n, across), far_r.at[n - half], far_sem.at[0, n], far_sem.at[1, n], down)
        for n in range(chunks)
    ]
    to_up = [send(block(n, up), near_l.at[n], near_sem.at[0, n], near_sem.at[1, n], up) for n in range(chunks)]
    to_down = [send(block(n, down), near_r.at[n], near_sem.at[2, n], near_sem.at[3, n], down) for n in range(chunks)]

    for i, n in enumerate(order):
        cols = slice(n * CHUNK, n * CHUNK + CHUNK)
        terms[n] = mul3(combined[...], jnp.concatenate([slab[:, cols], w_prev[:, cols]], axis=0))
        if i == 0:
            pl.semaphore_wait(barrier, 2)
        far[n].start()
    for i in range(half):
        to_up[half + i].start()
        to_down[i].start()
    for i in range(half):
        far[i].wait_recv()
        spot = pl.ds(pl.multiple_of(up * rows, 8), rows)
        terms[i, spot, :] = terms[i, spot, :] + far_l[i]
        to_up[i].start()
        far[half + i].wait_recv()
        spot = pl.ds(pl.multiple_of(down * rows, 8), rows)
        terms[half + i, spot, :] = terms[half + i, spot, :] + far_r[i]
        to_down[half + i].start()
    own = pl.ds(pl.multiple_of(y * rows, 8), rows)
    for i in range(half):
        for n in (i, half + i):
            to_up[n].wait_recv()
            to_down[n].wait_recv()
            out[:, n * CHUNK : n * CHUNK + CHUNK] = terms[n, own, :] + (near_l[n] + near_r[n])
    for copy in far + to_up + to_down:
        copy.wait_send()


def core_product(combined, slab, w_prev):
    cols = slab.shape[1]
    chunks = cols // CHUNK
    rows = K // NY
    vmem = pl.BlockSpec(memory_space=pltpu.VMEM)
    f32 = jnp.float32
    dma = pltpu.SemaphoreType.DMA
    return pl.pallas_call(
        core_kernel,
        out_shape=jax.ShapeDtypeStruct((rows, cols), f32),
        in_specs=[vmem, vmem, vmem],
        out_specs=vmem,
        scratch_shapes=[
            pltpu.VMEM((chunks, K, CHUNK), f32),
            pltpu.VMEM((chunks // 2, rows, CHUNK), f32),
            pltpu.VMEM((chunks // 2, rows, CHUNK), f32),
            pltpu.VMEM((chunks, rows, CHUNK), f32),
            pltpu.VMEM((chunks, rows, CHUNK), f32),
            dma((2, chunks)),
            dma((4, chunks)),
        ],
        compiler_params=pltpu.CompilerParams(collective_id=1, has_side_effects=True, vmem_limit_bytes=40 * 2**20),
        cost_estimate=pl.CostEstimate(flops=60_000_000_000, bytes_accessed=10_000_000, transcendentals=0),
        name="core_product",
    )(combined, slab, w_prev)


def on_device(slab, omega, y_prev, w_prev, prev_bucket, prev_sign, slab_bucket, slab_sign):
    gathered = sums(slab, omega, y_prev, prev_bucket, prev_sign, slab_bucket, slab_sign)
    q_prev, q_new, combined = factors(gathered, y_prev)
    return (q_prev, q_new, core_product(combined, slab, w_prev))


def solution(mesh):
    finer = Mesh(mesh.devices.reshape(NZ, NX, NC, NY), ("z", "x", "core", "y"))
    return jax.shard_map(
        on_device,
        mesh=finer,
        in_specs=(
            P("y", COL),
            P(COL, None),
            P(ROW_COL, None),
            P("y", COL),
            P(ROW_COL),
            P(ROW_COL),
            P("y"),
            P("y"),
        ),
        out_specs=(P(ROW_COL, None), P(ROW_COL, None), P("y", COL)),
        check_vma=False,
    )
```

```python
import jax
import jax.numpy as jnp
from jax import lax
from jax.experimental import pallas as pl
from jax.experimental.pallas import tpu as pltpu
from jax.sharding import Mesh
from jax.sharding import PartitionSpec as P

L = 512
COL = ("z", "x", "core")
ROW_COL = ("y", "z", "x", "core")
MESH = pl.DeviceIdType.MESH
highest = lax.Precision.HIGHEST
K = 256
BLK = 16
SUP = 64


def mm(a, b, dims=((1,), (0,))):
    return lax.dot_general(a, b, (dims, ((), ())), precision=highest, preferred_element_type=jnp.float32)


def eliminate(panel, k):
    off = k * BLK
    tile = off // 128 * 128
    cols = []
    for j in range(BLK):
        c = off + j
        cols.append([jnp.broadcast_to(panel[h * 8 : h * 8 + 8, c : c + 1], (8, 128)) for h in (0, 1)])
    lane = lax.broadcasted_iota(jnp.int32, (8, K), 1)
    row = lax.broadcasted_iota(jnp.int32, (8, K), 0)
    row1 = lax.broadcasted_iota(jnp.int32, (8, 128), 0)
    inside = (lane >= off) & (lane < off + BLK)
    top = jnp.where(inside, (lane == row + off).astype(jnp.float32), panel[:8])
    bot = jnp.where(inside, (lane == row + off + 8).astype(jnp.float32), panel[8:])
    lane1 = lax.broadcasted_iota(jnp.int32, (8, 128), 1) + tile
    corner = [jnp.zeros((8, 128), jnp.float32), jnp.zeros((8, 128), jnp.float32)]
    scales = []
    for j in range(BLK):
        h, r = divmod(j, 8)
        mine = cols[j]
        pivot = jnp.broadcast_to(mine[h][r : r + 1], (8, 128))
        rs = lax.rsqrt(pivot)
        inv = rs * rs
        scales.append(rs)
        low = mine[1] * inv
        high = None
        if h == 0:
            high = mine[0] * inv
        for m in range(j + 1, BLK):
            hm, rm = divmod(m, 8)
            u = jnp.broadcast_to(mine[hm][rm : rm + 1], (8, 128))
            cols[m][1] = cols[m][1] - low * u
            if hm == 0:
                cols[m][0] = cols[m][0] - high * u
        if h == 0:
            p = jnp.broadcast_to(top[r : r + 1], (8, K))
            hm_ = jnp.where(row1 > r, high, 0.0)
            top = top - jnp.concatenate([hm_, hm_], axis=1) * p
            bot = bot - jnp.concatenate([low, low], axis=1) * p
        else:
            p = jnp.broadcast_to(bot[r : r + 1], (8, K))
            lm_ = jnp.where(row1 > r, low, 0.0)
            bot = bot - jnp.concatenate([lm_, lm_], axis=1) * p
    st = jnp.zeros((8, 128), jnp.float32)
    sb = jnp.zeros((8, 128), jnp.float32)
    for j in range(8):
        st = jnp.where(row1 == j, scales[j], st)
        sb = jnp.where(row1 == j, scales[j + 8], sb)
    top = top * jnp.concatenate([st, st], axis=1)
    bot = bot * jnp.concatenate([sb, sb], axis=1)
    for j in range(BLK):
        for h in (0, 1):
            keep = (lane1 == off + j) & (row1 + 8 * h >= j)
            corner[h] = jnp.where(keep, cols[j][h] * scales[j], corner[h])
    return jnp.concatenate([top, bot], axis=0), jnp.concatenate(corner, axis=0)


def factor_step(w, u, k):
    off = k * BLK
    rows = slice(off, off + BLK)
    panel, corner = eliminate(w[rows, :], k)
    tile = off // 128 * 128
    w[rows, :] = panel
    lane = lax.broadcasted_iota(jnp.int32, (BLK, K), 1)
    upper = jnp.where(lane >= off + BLK, panel, 0.0)
    u[rows, :] = upper
    sup_end = (off // SUP + 1) * SUP
    if off + BLK < sup_end:
        turned = panel[:, tile : tile + 128].T
        left = turned[off + BLK - tile : sup_end - tile]
        rest = slice(off + BLK, sup_end)
        lane2 = lax.broadcasted_iota(jnp.int32, (sup_end - off - BLK, K), 1)
        old = jnp.where((lane2 >= off) & (lane2 < off + BLK), 0.0, w[rest, :])
        w[rest, :] = old - mm(left, panel)
    elif sup_end < K:
        start = sup_end - SUP
        block = w[start:sup_end, :]
        t0 = sup_end // 128 * 128
        turned = block[:, t0:].T
        left = turned[sup_end - t0 :]
        rest = slice(sup_end, K)
        lane2 = lax.broadcasted_iota(jnp.int32, (K - sup_end, K), 1)
        old = jnp.where((lane2 >= start) & (lane2 < sup_end), 0.0, w[rest, :])
        lane3 = lax.broadcasted_iota(jnp.int32, (SUP, K), 1)
        row3 = lax.broadcasted_iota(jnp.int32, (SUP, K), 0) + start
        block = jnp.where((lane3 < sup_end) & (lane3 > row3), 0.0, block)
        w[rest, :] = old - mm(left, block)
    return corner


def factor_both(wg, ws, ug, us, after):
    for k in range(K // BLK):
        cg = factor_step(wg, ug, k)
        factor_step(ws, us, k)
        off = k * BLK
        tile = off // 128 * 128
        rows = slice(off, off + BLK)
        turned = cg.T[off - tile : off - tile + BLK]
        ug[rows, off:off + BLK] = turned
        after(k)


NZ, NX, NC, NY = 8, 4, 2, 4
CHUNK = 512
SUMS = L + K
PART_A = SUMS // 2 // NY
PART_B = PART_A // NX
PIECE = K // NX
BLOCK = PIECE + 2 * PART_B + 8


def split(v):
    high = v.astype(jnp.bfloat16)
    return high, (v - high.astype(jnp.float32)).astype(jnp.bfloat16)


def mul(a, b, dims=((1,), (0,))):
    return lax.dot_general(a, b, (dims, ((), ())), preferred_element_type=jnp.float32)


def mul3(a, b, dims=((1,), (0,))):
    ah, al = split(a)
    bh, bl = split(b)
    return mul(ah, bh, dims) + (mul(ah, bl, dims) + mul(al, bh, dims))


def signed_sum(table, v):
    high = v.astype(jnp.bfloat16)
    rest = v - high.astype(jnp.float32)
    mid = rest.astype(jnp.bfloat16)
    low = (rest - mid.astype(jnp.float32)).astype(jnp.bfloat16)
    return mul(table, high) + (mul(table, mid) + mul(table, low))


def table_of(bucket, sign):
    level = lax.broadcasted_iota(jnp.int32, (L, bucket.shape[1]), 0).astype(jnp.float32)
    return jnp.where(level == bucket, 2.0 * sign - 1.0, 0.0).astype(jnp.bfloat16)


def whole_kernel(slab, omega, y_prev, w_prev, prev_bucket, prev_sign, slab_bucket, slab_sign, q_prev, q_new, x_core,
                 out, slab_v, omega_v, w_v, stack, part, got_sums, got_part, chip_sums, chip_part, got_a, got_b, got_s,
                 got_c, got_z, mid_p, mid_a, mid_s, xg, xs, u, us, ys, zs, ts, comb, comb_v, core, mapping,
                 early, v_far, v_up, v_down, terms, far_l, far_r, near_l, near_r, found_v, pass_up, pass_down,
                 load_sem, swap_sem, a_sem, b_sem, s_sem, c_sem, z_sem, d_sem, e_sem, f_sem, g_sem, v_sem, x_sem, far_sem, near_sem):
    z, x, c, y = (lax.axis_index(name) for name in ("z", "x", "core", "y"))

    def at(dz=0, dx=0, dc=0, dy=0):
        return {"z": (z + dz) % NZ, "x": (x + dx) % NX, "core": (c + dc) % NC, "y": (y + dy) % NY}

    def send(src, dst, sems, i, where):
        copy = pltpu.make_async_remote_copy(
            src_ref=src, dst_ref=dst, send_sem=sems.at[0, i], recv_sem=sems.at[1, i], device_id=where, device_id_type=MESH
        )
        copy.start()
        return copy

    barrier = pltpu.get_barrier_semaphore()
    peers = [at(dz=d) for d in range(1, NZ)]
    peers += [at(dy=d) for d in range(1, NY)] + [at(dx=d) for d in range(1, NX)] + [at(dc=1)]
    for peer in peers:
        pl.semaphore_signal(barrier, inc=1, device_id=peer, device_id_type=MESH)

    chunks = slab_v.shape[0]
    loads = []
    for i in range(chunks):
        loads.append(pltpu.make_async_copy(slab.at[:, pl.ds(i * CHUNK, CHUNK)], slab_v.at[i], load_sem.at[0, i]))
        loads.append(pltpu.make_async_copy(omega.at[pl.ds(i * CHUNK, CHUNK), :], omega_v.at[i], load_sem.at[1, i]))
    for load in loads:
        load.start()
    for i in range(chunks):
        pltpu.make_async_copy(w_prev.at[:, pl.ds(i * CHUNK, CHUNK)], w_v.at[i], load_sem.at[2, i]).start()

    def real(ref):
        return ref[...].astype(jnp.float32)

    bucket, sign = real(prev_bucket), real(prev_sign)
    table = jnp.concatenate([table_of(bucket[h : h + 1], sign[h : h + 1]) for h in (0, 1)], axis=1)
    own = y_prev[...]
    stack[:L, :] = signed_sum(table, own)
    stack[L:, :] = mm(own, own, ((0,), (0,)))
    out[c, y, x, PIECE + 2 * PART_B :, :] = jnp.concatenate([real(slab_bucket), real(slab_sign), jnp.zeros((4, 128), jnp.float32)])
    part[...] = jnp.zeros_like(part)

    def multiply(i):
        pltpu.make_async_copy(slab.at[:, pl.ds(0, CHUNK)], slab_v.at[i], load_sem.at[0, i]).wait()
        pltpu.make_async_copy(omega.at[pl.ds(0, CHUNK), :], omega_v.at[i], load_sem.at[1, i]).wait()
        part[...] += mul3(slab_v[i], omega_v[i])

    pl.loop(0, chunks)(multiply)
    pl.semaphore_wait(barrier, len(peers))

    ours = pl.ds(pl.multiple_of(c * 128, 128), 128)
    theirs = pl.ds(pl.multiple_of((1 - c) * 128, 128), 128)
    swap_sums = send(stack.at[:, theirs], got_sums, swap_sem, 0, at(dc=1))
    swap_part = send(part.at[:, theirs], got_part, swap_sem, 1, at(dc=1))

    def share(half, where):
        place = where["x"] if half else where["y"]
        return pl.ds(pl.multiple_of(half * (SUMS // 2) + place * PART_A, 8), PART_A)

    swap_sums.wait_recv()
    chip_sums[...] = stack[:, ours] + got_sums[...]
    sent_a = []
    for d in (2, 1, 3):
        for half in (0, 1):
            where = at(dx=d) if half else at(dy=d)
            sent_a.append(send(chip_sums.at[share(half, where), :], got_a.at[half, d - 1], a_sem, 2 * (d - 1) + half, where))

    swap_part.wait_recv()
    chip_part[...] = part[:, ours] + got_part[...]
    sent_b = []
    for d in (2, 1, 3):
        where = at(dx=d)
        piece = chip_part.at[pl.ds(pl.multiple_of(where["x"] * PIECE, 8), PIECE), :]
        sent_b.append(send(piece, got_b.at[d - 1], b_sem, d - 1, where))

    for copy in sent_a:
        copy.wait_recv()
    for half in (0, 1):
        total = chip_sums[share(half, at()), :]
        for d in range(1, 4):
            total = total + got_a[half, d - 1]
        mid_a[half] = total
    sent_s = []
    for d in range(1, NX):
        for half in (0, 1):
            where = at(dy=d) if half else at(dx=d)
            place = where["y"] if half else where["x"]
            piece = mid_a.at[half, pl.ds(pl.multiple_of(place * PART_B, 8), PART_B), :]
            sent_s.append(send(piece, got_s.at[half, d - 1], s_sem, 2 * (d - 1) + half, where))

    for copy in sent_b:
        copy.wait_recv()
    total = chip_part[pl.ds(pl.multiple_of(x * PIECE, 8), PIECE), :]
    for d in range(1, NX):
        total = total + got_b[d - 1]
    mid_p[...] = total
    sent_c = []
    for d in range(1, NZ):
        where = at(dz=d)
        piece = mid_p.at[pl.ds(pl.multiple_of(where["z"] * 8, 8), 8), :]
        sent_c.append(send(piece, got_c.at[d - 1], c_sem, d - 1, where))

    for copy in sent_s:
        copy.wait_recv()
    for half in (0, 1):
        total = mid_a[half, pl.ds(pl.multiple_of((y if half else x) * PART_B, 8), PART_B), :]
        for d in range(1, NX):
            total = total + got_s[half, d - 1]
        mid_s[half * PART_B : half * PART_B + PART_B, :] = total
    sent_z = [send(mid_s, got_z.at[d - 1], z_sem, d - 1, at(dz=d)) for d in range(1, NZ)]

    for copy in sent_c:
        copy.wait_recv()
    total = mid_p[pl.ds(pl.multiple_of(z * 8, 8), 8), :]
    for d in range(1, NZ):
        total = total + got_c[d - 1]
    tile = pl.ds(pl.multiple_of(z * 8, 8), 8)
    out[c, y, x, tile, :] = total
    sent_d = [send(out.at[c, y, x, tile, :], out.at[c, y, x, tile, :], d_sem, d - 1, at(dz=d)) for d in range(1, NZ)]

    for copy in sent_z:
        copy.wait_recv()
    total = mid_s[...]
    for d in range(1, NZ):
        total = total + got_z[d - 1]
    out[c, y, x, PIECE : PIECE + 2 * PART_B, :] = total
    for copy in sent_d:
        copy.wait_recv()

    def first(d):
        return at(dx=d * (1 - c), dy=d * c)

    def second(d):
        return at(dx=d * c, dy=d * (1 - c))

    def gathered(n, d):
        return out.at[c, (y + (4 - n) * c + (4 - d) * (1 - c)) % NY, (x + (4 - n) * (1 - c) + (4 - d) * c) % NX]

    def swap(n, d):
        block = gathered(n, d)
        return send(block, block, g_sem, 4 * n + d, at(dc=1))

    def both_ways(n):
        block = gathered(n, 0)
        return [send(block, block, f_sem, 3 * n + d - 1, second(d)) for d in (1, 3)]

    own_block = gathered(0, 0)
    sent_e = [send(own_block, own_block, e_sem, d - 1, first(d)) for d in range(1, 4)]
    sent_f = {0: both_ways(0)}
    sent_g = [swap(0, 0)]
    for n in (1, 3, 2):
        sent_e[n - 1].wait_recv()
        sent_f[n] = both_ways(n)
        sent_g.append(swap(n, 0))
    passed = []
    for n in (0, 1, 3, 2):
        for d in (1, 3):
            sent_f[n][d // 2].wait_recv()
            block = gathered(n, d)
            if d == (1, 3)[n % 2]:
                passed.append((n, send(block, block, f_sem, 3 * n + 1, second(d))))
            sent_g.append(swap(n, d))
    for n, copy in passed:
        copy.wait_recv()
        sent_g.append(swap(n, 2))
    sent_f = [copy for n in range(4) for copy in sent_f[n]] + [copy for _, copy in passed]
    for copy in sent_g:
        copy.wait_recv()
    everything = [swap_sums, swap_part] + sent_a + sent_b + sent_s + sent_c + sent_z + sent_d + sent_e + sent_f + sent_g

    for cc in range(NC):
        lanes = slice(128 * cc, 128 * cc + 128)
        for yy in range(NY):
            for xx in range(NX):
                ys[pl.ds(256 * yy + PIECE * xx, PIECE), lanes] = out[cc, yy, xx, :PIECE, :]
                for half in (0, 1):
                    start = half * (SUMS // 2) + (PART_A * xx + PART_B * yy if half else PART_A * yy + PART_B * xx)
                    zs[pl.ds(start, PART_B), lanes] = out[cc, yy, xx, PIECE + half * PART_B : PIECE + half * PART_B + PART_B, :]
    for yy in range(NY):
        marks = out[0, yy, 0, PIECE + 2 * PART_B :, :]
        for h in (0, 1):
            ts[yy, :, 128 * h : 128 * h + 128] = table_of(marks[h : h + 1], marks[h + 2 : h + 3])
    new = ys[...]
    xg[...] = zs[L:, :] + mm(new, new, ((0,), (0,)))
    sketch = zs[:L, :]
    for yy in range(NY):
        sketch = sketch + signed_sum(ts[yy], ys[256 * yy : 256 * yy + 256, :])
    zs[:L, :] = sketch

    up, across, down = (y + 1) % NY, (y + 2) % NY, (y + 3) % NY
    mine = pl.ds(pl.multiple_of(y * 128, 128), 128)
    for i in range(chunks):
        pltpu.make_async_copy(w_prev.at[:, pl.ds(0, CHUNK)], w_v.at[i], load_sem.at[2, i]).wait()
    high = sketch.astype(jnp.bfloat16)
    rest = sketch - high.astype(jnp.float32)
    mid = rest.astype(jnp.bfloat16)
    low = (rest - mid.astype(jnp.float32)).astype(jnp.bfloat16)
    table = ts[y]
    over = ((0,), (0,))
    comb_v[:, :256] = mul(high, table, over) + (mul(mid, table, over) + mul(low, table, over))
    comb_v[:, 256:] = zs[mine, :].T

    def data(n):
        return jnp.concatenate([slab_v[n], w_v[n]], axis=0)

    def along(src, dst, sems, i, peer):
        return send(src, dst, sems, i, at(dy=peer))

    front, back = slice(0, K // 2), slice(K // 2, K)
    early[2] = mul3(comb_v[...], data(across))
    moves = [
        along(early.at[2, front, :], v_far.at[0], v_sem, 0, 1),
        along(early.at[2, back, :], v_far.at[1], v_sem, 1, 3),
    ]
    early[1] = mul3(comb_v[...], data(up))
    moves.append(along(early.at[1, back, :], v_up.at[back, :], v_sem, 2, 1))
    early[3] = mul3(comb_v[...], data(down))
    moves.append(along(early.at[3, front, :], v_down.at[front, :], v_sem, 3, 3))
    early[0] = mul3(comb_v[...], data(y))

    def after(k):
        if k != 10:
            return
        moves[0].wait_recv()
        early[1, front, :] = early[1, front, :] + v_far[0]
        moves.append(along(early.at[1, front, :], v_up.at[front, :], v_sem, 4, 1))
        moves[1].wait_recv()
        early[3, back, :] = early[3, back, :] + v_far[1]
        moves.append(along(early.at[3, back, :], v_down.at[back, :], v_sem, 5, 3))

    xs[...] = mm(sketch, sketch, over)
    factor_both(xg, xs, u, us, after)
    row = lax.broadcasted_iota(jnp.int32, (K, K), 0)
    lane = lax.broadcasted_iota(jnp.int32, (K, K), 1)
    inner = jnp.where(lane <= row, xs[...], 0.0)
    core[...] = mm(mm(u[...], inner, ((1,), (1,))), inner)
    found = mm(core[...], zs[:L, :], ((1,), (1,)))
    mapping[...] = found
    high = found.astype(jnp.bfloat16)
    rest = found - high.astype(jnp.float32)
    mid = rest.astype(jnp.bfloat16)
    low = (rest - mid.astype(jnp.float32)).astype(jnp.bfloat16)
    table = ts[y]
    comb[:, :256] = mul(high, table) + (mul(mid, table) + mul(low, table))
    comb[:, 256:] = mapping[:, mine]

    rows = x_core.shape[0]
    late = chunks - NY
    half = late // 2

    def spot(place):
        return pl.ds(pl.multiple_of(place * rows, 8), rows)

    far = {}
    for n in [n for i in range(half) for n in (i, half + i)]:
        terms[n] = mul3(comb[...], data(NY + n))
        left = n < half
        far[n] = along(terms.at[n, spot(across), :], far_l.at[n] if left else far_r.at[n - half], far_sem, n, 1 if left else 3)
    to_up, to_down = {}, {}

    def near(n, upward):
        if upward:
            to_up[n] = along(terms.at[n, spot(up), :], near_l.at[n], near_sem, n, 1)
        else:
            to_down[n] = along(terms.at[n, spot(down), :], near_r.at[n], near_sem, late + n, 3)

    for i in range(half):
        near(half + i, True)
        near(i, False)

    for copy in moves[2:]:
        copy.wait_recv()
    found_v[...] = mm(core[...], early[0] + (v_up[...] + v_down[...]))

    def columns(place, start, size):
        return pl.ds(pl.multiple_of(place * CHUNK + start, 128), size)

    wide = CHUNK // 2
    relay_up = along(found_v.at[spot(across), 0:wide], pass_up, x_sem, 0, 1)
    relay_down = along(found_v.at[spot(across), wide:CHUNK], pass_down, x_sem, 1, 3)
    home = [
        along(found_v.at[spot(up), :], x_core.at[:, columns(y, 0, CHUNK)], x_sem, 2, 1),
        along(found_v.at[spot(down), :], x_core.at[:, columns(y, 0, CHUNK)], x_sem, 3, 3),
    ]
    for i in range(half):
        far[i].wait_recv()
        terms[i, spot(up), :] = terms[i, spot(up), :] + far_l[i]
        near(i, True)
        far[half + i].wait_recv()
        terms[half + i, spot(down), :] = terms[half + i, spot(down), :] + far_r[i]
        near(half + i, False)
    relay_up.wait_recv()
    home.append(along(pass_up, x_core.at[:, columns(down, 0, wide)], x_sem, 4, 1))
    relay_down.wait_recv()
    home.append(along(pass_down, x_core.at[:, columns(up, wide, wide)], x_sem, 5, 3))
    x_core[:, columns(y, 0, CHUNK)] = found_v[spot(y), :]

    outer = jnp.where(lane <= row, xg[...], 0.0)
    q_prev[...] = mm(y_prev[...], outer, ((1,), (1,)))
    col = (z * NX + x) * NC + c
    pair = mm(ys[pl.ds(pl.multiple_of(y * 256 + (col // 2) * 8, 8), 8), :], outer, ((1,), (1,)))
    q_new[...] = jnp.where(col % 2 == 0, pair[:4], pair[4:])

    for i in range(half):
        for n in (half + i, i):
            to_up[n].wait_recv()
            to_down[n].wait_recv()
            x_core[:, (NY + n) * CHUNK : (NY + n + 1) * CHUNK] = terms[n, spot(y), :] + (near_l[n] + near_r[n])
    for copy in home:
        copy.wait_recv()
    everything += moves + [relay_up, relay_down] + home + list(far.values()) + list(to_up.values()) + list(to_down.values())
    for copy in everything:
        copy.wait_send()


def whole(slab, omega, y_prev, w_prev, *marks):
    rows, cols = slab.shape
    chunks = cols // CHUNK
    late = chunks - NY
    share = K // NY
    vmem = pl.BlockSpec(memory_space=pltpu.VMEM)
    hbm = pl.BlockSpec(memory_space=pltpu.HBM)
    f32 = jnp.float32
    dma = pltpu.SemaphoreType.DMA

    def buffers(*shapes):
        return [pltpu.VMEM(shape, f32) for shape in shapes]

    return pl.pallas_call(
        whole_kernel,
        out_shape=(
            jax.ShapeDtypeStruct(y_prev.shape, f32),
            jax.ShapeDtypeStruct((4, K), f32),
            jax.ShapeDtypeStruct((share, cols), f32),
        ),
        in_specs=[hbm, hbm, vmem, hbm] + [vmem] * 4,
        out_specs=[vmem] * 3,
        scratch_shapes=buffers(
            (NC, NY, NX, BLOCK, 128),
            (chunks, rows, CHUNK),
            (chunks, CHUNK, K),
            (chunks, w_prev.shape[0], CHUNK),
            (SUMS, K),
            (rows, K),
            (SUMS, 128),
            (rows, 128),
            (SUMS, 128),
            (rows, 128),
            (2, 3, PART_A, 128),
            (3, PIECE, 128),
            (2, 3, PART_B, 128),
            (7, 8, 128),
            (7, 2 * PART_B, 128),
            (PIECE, 128),
            (2, PART_A, 128),
            (2 * PART_B, 128),
            (K, K),
            (K, K),
            (K, K),
            (K, K),
            (1024, K),
            (SUMS, K),
        )
        + [pltpu.VMEM((NY, L, K), jnp.bfloat16)]
        + buffers(
            (K, 384),
            (K, 384),
            (K, K),
            (K, L),
            (NY, K, CHUNK),
            (2, K // 2, CHUNK),
            (K, CHUNK),
            (K, CHUNK),
            (late, K, CHUNK),
            (late // 2, share, CHUNK),
            (late // 2, share, CHUNK),
            (late, share, CHUNK),
            (late, share, CHUNK),
            (K, CHUNK),
            (share, CHUNK // 2),
            (share, CHUNK // 2),
        )
        + [
            dma((3, chunks)),
            dma((2, 2)),
            dma((2, 6)),
            dma((2, 3)),
            dma((2, 6)),
            dma((2, 7)),
            dma((2, 7)),
            dma((2, 7)),
            dma((2, 3)),
            dma((2, 12)),
            dma((2, 16)),
            dma((2, 6)),
            dma((2, 6)),
            dma((2, late)),
            dma((2, 2 * late)),
        ],
        compiler_params=pltpu.CompilerParams(collective_id=0, has_side_effects=True, vmem_limit_bytes=67_043_328),
        cost_estimate=pl.CostEstimate(flops=60_000_000_000, bytes_accessed=20_000_000, transcendentals=0),
        name="whole",
    )(slab, omega, y_prev, w_prev, *(mark.reshape(2, 128) for mark in marks))


def solution(mesh):
    finer = Mesh(mesh.devices.reshape(NZ, NX, NC, NY), ("z", "x", "core", "y"))
    return jax.shard_map(
        whole,
        mesh=finer,
        in_specs=(
            P("y", COL),
            P(COL, None),
            P(ROW_COL, None),
            P("y", COL),
            P(ROW_COL),
            P(ROW_COL),
            P("y"),
            P("y"),
        ),
        out_specs=(P(ROW_COL, None), P(ROW_COL, None), P("y", COL)),
        check_vma=False,
    )
```

```python
import jax
import jax.numpy as jnp
from jax import lax
from jax.experimental import pallas as pl
from jax.experimental.pallas import tpu as pltpu
from jax.sharding import Mesh
from jax.sharding import PartitionSpec as P

L = 512
COL = ("z", "x", "core")
ROW_COL = ("y", "z", "x", "core")
MESH = pl.DeviceIdType.MESH
highest = lax.Precision.HIGHEST
K = 256
BLK = 16
SUP = 64


def mm(a, b, dims=((1,), (0,))):
    return lax.dot_general(a, b, (dims, ((), ())), precision=highest, preferred_element_type=jnp.float32)


def eliminate(panel, k):
    off = k * BLK
    tile = off // 128 * 128
    cols = []
    for j in range(BLK):
        c = off + j
        cols.append([jnp.broadcast_to(panel[h * 8 : h * 8 + 8, c : c + 1], (8, 128)) for h in (0, 1)])
    lane = lax.broadcasted_iota(jnp.int32, (8, K), 1)
    row = lax.broadcasted_iota(jnp.int32, (8, K), 0)
    row1 = lax.broadcasted_iota(jnp.int32, (8, 128), 0)
    inside = (lane >= off) & (lane < off + BLK)
    top = jnp.where(inside, (lane == row + off).astype(jnp.float32), panel[:8])
    bot = jnp.where(inside, (lane == row + off + 8).astype(jnp.float32), panel[8:])
    lane1 = lax.broadcasted_iota(jnp.int32, (8, 128), 1) + tile
    corner = [jnp.zeros((8, 128), jnp.float32), jnp.zeros((8, 128), jnp.float32)]
    scales = []
    for j in range(BLK):
        h, r = divmod(j, 8)
        mine = cols[j]
        pivot = jnp.broadcast_to(mine[h][r : r + 1], (8, 128))
        rs = lax.rsqrt(pivot)
        inv = rs * rs
        scales.append(rs)
        low = mine[1] * inv
        high = None
        if h == 0:
            high = mine[0] * inv
        for m in range(j + 1, BLK):
            hm, rm = divmod(m, 8)
            u = jnp.broadcast_to(mine[hm][rm : rm + 1], (8, 128))
            cols[m][1] = cols[m][1] - low * u
            if hm == 0:
                cols[m][0] = cols[m][0] - high * u
        if h == 0:
            p = jnp.broadcast_to(top[r : r + 1], (8, K))
            hm_ = jnp.where(row1 > r, high, 0.0)
            top = top - jnp.concatenate([hm_, hm_], axis=1) * p
            bot = bot - jnp.concatenate([low, low], axis=1) * p
        else:
            p = jnp.broadcast_to(bot[r : r + 1], (8, K))
            lm_ = jnp.where(row1 > r, low, 0.0)
            bot = bot - jnp.concatenate([lm_, lm_], axis=1) * p
    st = jnp.zeros((8, 128), jnp.float32)
    sb = jnp.zeros((8, 128), jnp.float32)
    for j in range(8):
        st = jnp.where(row1 == j, scales[j], st)
        sb = jnp.where(row1 == j, scales[j + 8], sb)
    top = top * jnp.concatenate([st, st], axis=1)
    bot = bot * jnp.concatenate([sb, sb], axis=1)
    for j in range(BLK):
        for h in (0, 1):
            keep = (lane1 == off + j) & (row1 + 8 * h >= j)
            corner[h] = jnp.where(keep, cols[j][h] * scales[j], corner[h])
    return jnp.concatenate([top, bot], axis=0), jnp.concatenate(corner, axis=0)


def factor_step(w, u, k):
    off = k * BLK
    rows = slice(off, off + BLK)
    panel, corner = eliminate(w[rows, :], k)
    tile = off // 128 * 128
    w[rows, :] = panel
    lane = lax.broadcasted_iota(jnp.int32, (BLK, K), 1)
    upper = jnp.where(lane >= off + BLK, panel, 0.0)
    u[rows, :] = upper
    sup_end = (off // SUP + 1) * SUP
    if off + BLK < sup_end:
        turned = panel[:, tile : tile + 128].T
        left = turned[off + BLK - tile : sup_end - tile]
        rest = slice(off + BLK, sup_end)
        lane2 = lax.broadcasted_iota(jnp.int32, (sup_end - off - BLK, K), 1)
        old = jnp.where((lane2 >= off) & (lane2 < off + BLK), 0.0, w[rest, :])
        w[rest, :] = old - mm(left, panel)
    elif sup_end < K:
        start = sup_end - SUP
        block = w[start:sup_end, :]
        t0 = sup_end // 128 * 128
        turned = block[:, t0:].T
        left = turned[sup_end - t0 :]
        rest = slice(sup_end, K)
        lane2 = lax.broadcasted_iota(jnp.int32, (K - sup_end, K), 1)
        old = jnp.where((lane2 >= start) & (lane2 < sup_end), 0.0, w[rest, :])
        lane3 = lax.broadcasted_iota(jnp.int32, (SUP, K), 1)
        row3 = lax.broadcasted_iota(jnp.int32, (SUP, K), 0) + start
        block = jnp.where((lane3 < sup_end) & (lane3 > row3), 0.0, block)
        w[rest, :] = old - mm(left, block)
    return corner


def factor_both(wg, ws, ug, us, after):
    for k in range(K // BLK):
        cg = factor_step(wg, ug, k)
        factor_step(ws, us, k)
        off = k * BLK
        tile = off // 128 * 128
        rows = slice(off, off + BLK)
        turned = cg.T[off - tile : off - tile + BLK]
        ug[rows, off:off + BLK] = turned
        after(k)


NZ, NX, NC, NY = 8, 4, 2, 4
CHUNK = 512
SUMS = L + K
PART_A = SUMS // 2 // NY
PART_B = PART_A // NX
PIECE = K // NX
BLOCK = PIECE + 2 * PART_B + 8


def split(v):
    high = v.astype(jnp.bfloat16)
    return high, (v - high.astype(jnp.float32)).astype(jnp.bfloat16)


def mul(a, b, dims=((1,), (0,))):
    return lax.dot_general(a, b, (dims, ((), ())), preferred_element_type=jnp.float32)


def mul3(a, b, dims=((1,), (0,))):
    ah, al = split(a)
    bh, bl = split(b)
    return mul(ah, bh, dims) + (mul(ah, bl, dims) + mul(al, bh, dims))


def signed_sum(table, v):
    high = v.astype(jnp.bfloat16)
    rest = v - high.astype(jnp.float32)
    mid = rest.astype(jnp.bfloat16)
    low = (rest - mid.astype(jnp.float32)).astype(jnp.bfloat16)
    return mul(table, high) + (mul(table, mid) + mul(table, low))


def table_of(bucket, sign):
    level = lax.broadcasted_iota(jnp.int32, (L, bucket.shape[1]), 0).astype(jnp.float32)
    return jnp.where(level == bucket, 2.0 * sign - 1.0, 0.0).astype(jnp.bfloat16)


def whole_kernel(slab, omega, y_in, w_prev, pb_in, ps_in, sb_in, ss_in, q_prev, q_new, x_core,
                 out, slab_v, omega_v, w_v, stack, part, got_sums, got_part, chip_sums, chip_part, got_a, got_b, got_s,
                 got_c, got_z, mid_p, mid_a, mid_s, xg, xs, u, us, ys, zs, ts, comb, comb_v, core, mapping,
                 early, v_far, v_up, v_down, terms, far_l, far_r, near_l, near_r, found_v, pass_up, pass_down,
                 y_prev, prev_bucket, prev_sign, slab_bucket, slab_sign, small_sem, load_sem, swap_sem, a_sem, b_sem, s_sem, c_sem, z_sem, d_sem, e_sem, f_sem, g_sem, v_sem, x_sem, far_sem, near_sem):
    z, x, c, y = (lax.axis_index(name) for name in ("z", "x", "core", "y"))

    def at(dz=0, dx=0, dc=0, dy=0):
        return {"z": (z + dz) % NZ, "x": (x + dx) % NX, "core": (c + dc) % NC, "y": (y + dy) % NY}

    def send(src, dst, sems, i, where):
        copy = pltpu.make_async_remote_copy(
            src_ref=src, dst_ref=dst, send_sem=sems.at[0, i], recv_sem=sems.at[1, i], device_id=where, device_id_type=MESH
        )
        copy.start()
        return copy

    barrier = pltpu.get_barrier_semaphore()
    peers = [at(dz=d) for d in range(1, NZ)]
    peers += [at(dy=d) for d in range(1, NY)] + [at(dx=d) for d in range(1, NX)] + [at(dc=1)]
    for peer in peers:
        pl.semaphore_signal(barrier, inc=1, device_id=peer, device_id_type=MESH)

    small = [
        pltpu.make_async_copy(src, dst, small_sem.at[i])
        for i, (src, dst) in enumerate(
            zip((y_in, pb_in, ps_in, sb_in, ss_in), (y_prev, prev_bucket, prev_sign, slab_bucket, slab_sign))
        )
    ]
    for copy in small:
        copy.start()
    chunks = slab_v.shape[0]
    loads = []
    for i in range(chunks):
        loads.append(pltpu.make_async_copy(slab.at[:, pl.ds(i * CHUNK, CHUNK)], slab_v.at[i], load_sem.at[0, i]))
        loads.append(pltpu.make_async_copy(omega.at[pl.ds(i * CHUNK, CHUNK), :], omega_v.at[i], load_sem.at[1, i]))
    for load in loads:
        load.start()
    for i in range(chunks):
        pltpu.make_async_copy(w_prev.at[:, pl.ds(i * CHUNK, CHUNK)], w_v.at[i], load_sem.at[2, i]).start()

    for copy in small:
        copy.wait()

    def real(ref):
        return ref[...].astype(jnp.float32)

    bucket, sign = real(prev_bucket), real(prev_sign)
    table = jnp.concatenate([table_of(bucket[h : h + 1], sign[h : h + 1]) for h in (0, 1)], axis=1)
    own = y_prev[...]
    stack[:L, :] = signed_sum(table, own)
    stack[L:, :] = mm(own, own, ((0,), (0,)))
    out[c, y, x, PIECE + 2 * PART_B :, :] = jnp.concatenate([real(slab_bucket), real(slab_sign), jnp.zeros((4, 128), jnp.float32)])
    part[...] = jnp.zeros_like(part)

    def multiply(i):
        pltpu.make_async_copy(slab.at[:, pl.ds(0, CHUNK)], slab_v.at[i], load_sem.at[0, i]).wait()
        pltpu.make_async_copy(omega.at[pl.ds(0, CHUNK), :], omega_v.at[i], load_sem.at[1, i]).wait()
        part[...] += mul3(slab_v[i], omega_v[i])

    pl.loop(0, chunks)(multiply)
    pl.semaphore_wait(barrier, len(peers))

    ours = pl.ds(pl.multiple_of(c * 128, 128), 128)
    theirs = pl.ds(pl.multiple_of((1 - c) * 128, 128), 128)
    swap_sums = send(stack.at[:, theirs], got_sums, swap_sem, 0, at(dc=1))
    swap_part = send(part.at[:, theirs], got_part, swap_sem, 1, at(dc=1))

    def share(half, where):
        place = where["x"] if half else where["y"]
        return pl.ds(pl.multiple_of(half * (SUMS // 2) + place * PART_A, 8), PART_A)

    swap_sums.wait_recv()
    chip_sums[...] = stack[:, ours] + got_sums[...]
    sent_a = []
    for d in (2, 1, 3):
        for half in (0, 1):
            where = at(dx=d) if half else at(dy=d)
            sent_a.append(send(chip_sums.at[share(half, where), :], got_a.at[half, d - 1], a_sem, 2 * (d - 1) + half, where))

    swap_part.wait_recv()
    chip_part[...] = part[:, ours] + got_part[...]
    sent_b = []
    for d in (2, 1, 3):
        where = at(dx=d)
        piece = chip_part.at[pl.ds(pl.multiple_of(where["x"] * PIECE, 8), PIECE), :]
        sent_b.append(send(piece, got_b.at[d - 1], b_sem, d - 1, where))

    for copy in sent_a:
        copy.wait_recv()
    for half in (0, 1):
        total = chip_sums[share(half, at()), :]
        for d in range(1, 4):
            total = total + got_a[half, d - 1]
        mid_a[half] = total
    sent_s = []
    for d in range(1, NX):
        for half in (0, 1):
            where = at(dy=d) if half else at(dx=d)
            place = where["y"] if half else where["x"]
            piece = mid_a.at[half, pl.ds(pl.multiple_of(place * PART_B, 8), PART_B), :]
            sent_s.append(send(piece, got_s.at[half, d - 1], s_sem, 2 * (d - 1) + half, where))

    for copy in sent_b:
        copy.wait_recv()
    total = chip_part[pl.ds(pl.multiple_of(x * PIECE, 8), PIECE), :]
    for d in range(1, NX):
        total = total + got_b[d - 1]
    mid_p[...] = total
    sent_c = []
    for d in range(1, NZ):
        where = at(dz=d)
        piece = mid_p.at[pl.ds(pl.multiple_of(where["z"] * 8, 8), 8), :]
        sent_c.append(send(piece, got_c.at[d - 1], c_sem, d - 1, where))

    for copy in sent_s:
        copy.wait_recv()
    for half in (0, 1):
        total = mid_a[half, pl.ds(pl.multiple_of((y if half else x) * PART_B, 8), PART_B), :]
        for d in range(1, NX):
            total = total + got_s[half, d - 1]
        mid_s[half * PART_B : half * PART_B + PART_B, :] = total
    sent_z = [send(mid_s, got_z.at[d - 1], z_sem, d - 1, at(dz=d)) for d in range(1, NZ)]

    for copy in sent_c:
        copy.wait_recv()
    total = mid_p[pl.ds(pl.multiple_of(z * 8, 8), 8), :]
    for d in range(1, NZ):
        total = total + got_c[d - 1]
    tile = pl.ds(pl.multiple_of(z * 8, 8), 8)
    out[c, y, x, tile, :] = total
    sent_d = [send(out.at[c, y, x, tile, :], out.at[c, y, x, tile, :], d_sem, d - 1, at(dz=d)) for d in range(1, NZ)]

    for copy in sent_z:
        copy.wait_recv()
    total = mid_s[...]
    for d in range(1, NZ):
        total = total + got_z[d - 1]
    out[c, y, x, PIECE : PIECE + 2 * PART_B, :] = total
    for copy in sent_d:
        copy.wait_recv()

    def first(d):
        return at(dx=d * (1 - c), dy=d * c)

    def second(d):
        return at(dx=d * c, dy=d * (1 - c))

    def gathered(n, d):
        return out.at[c, (y + (4 - n) * c + (4 - d) * (1 - c)) % NY, (x + (4 - n) * (1 - c) + (4 - d) * c) % NX]

    def swap(n, d):
        block = gathered(n, d)
        return send(block, block, g_sem, 4 * n + d, at(dc=1))

    def both_ways(n):
        block = gathered(n, 0)
        return [send(block, block, f_sem, 3 * n + d - 1, second(d)) for d in (1, 3)]

    own_block = gathered(0, 0)
    sent_e = [send(own_block, own_block, e_sem, d - 1, first(d)) for d in range(1, 4)]
    sent_f = {0: both_ways(0)}
    sent_g = [swap(0, 0)]
    for n in (1, 3, 2):
        sent_e[n - 1].wait_recv()
        sent_f[n] = both_ways(n)
        sent_g.append(swap(n, 0))
    passed = []
    for n in (0, 1, 3, 2):
        for d in (1, 3):
            sent_f[n][d // 2].wait_recv()
            block = gathered(n, d)
            if d == (1, 3)[n % 2]:
                passed.append((n, send(block, block, f_sem, 3 * n + 1, second(d))))
            sent_g.append(swap(n, d))
    for n, copy in passed:
        copy.wait_recv()
        sent_g.append(swap(n, 2))
    sent_f = [copy for n in range(4) for copy in sent_f[n]] + [copy for _, copy in passed]
    for copy in sent_g:
        copy.wait_recv()
    everything = [swap_sums, swap_part] + sent_a + sent_b + sent_s + sent_c + sent_z + sent_d + sent_e + sent_f + sent_g

    for cc in range(NC):
        lanes = slice(128 * cc, 128 * cc + 128)
        for yy in range(NY):
            for xx in range(NX):
                ys[pl.ds(256 * yy + PIECE * xx, PIECE), lanes] = out[cc, yy, xx, :PIECE, :]
                for half in (0, 1):
                    start = half * (SUMS // 2) + (PART_A * xx + PART_B * yy if half else PART_A * yy + PART_B * xx)
                    zs[pl.ds(start, PART_B), lanes] = out[cc, yy, xx, PIECE + half * PART_B : PIECE + half * PART_B + PART_B, :]
    for yy in range(NY):
        marks = out[0, yy, 0, PIECE + 2 * PART_B :, :]
        for h in (0, 1):
            ts[yy, :, 128 * h : 128 * h + 128] = table_of(marks[h : h + 1], marks[h + 2 : h + 3])
    sketch = zs[:L, :]
    for yy in range(NY):
        sketch = sketch + signed_sum(ts[yy], ys[256 * yy : 256 * yy + 256, :])
    zs[:L, :] = sketch

    up, across, down = (y + 1) % NY, (y + 2) % NY, (y + 3) % NY
    mine = pl.ds(pl.multiple_of(y * 128, 128), 128)
    for i in range(chunks):
        pltpu.make_async_copy(w_prev.at[:, pl.ds(0, CHUNK)], w_v.at[i], load_sem.at[2, i]).wait()
    high = sketch.astype(jnp.bfloat16)
    rest = sketch - high.astype(jnp.float32)
    mid = rest.astype(jnp.bfloat16)
    low = (rest - mid.astype(jnp.float32)).astype(jnp.bfloat16)
    table = ts[y]
    over = ((0,), (0,))
    comb_v[:, :256] = mul(high, table, over) + (mul(mid, table, over) + mul(low, table, over))
    comb_v[:, 256:] = zs[mine, :].T

    def data(n):
        return jnp.concatenate([slab_v[n], w_v[n]], axis=0)

    def along(src, dst, sems, i, peer):
        return send(src, dst, sems, i, at(dy=peer))

    front, back = slice(0, K // 2), slice(K // 2, K)
    early[2] = mul3(comb_v[...], data(across))
    moves = [
        along(early.at[2, front, :], v_far.at[0], v_sem, 0, 1),
        along(early.at[2, back, :], v_far.at[1], v_sem, 1, 3),
    ]
    early[1] = mul3(comb_v[...], data(up))
    moves.append(along(early.at[1, back, :], v_up.at[back, :], v_sem, 2, 1))
    early[3] = mul3(comb_v[...], data(down))
    moves.append(along(early.at[3, front, :], v_down.at[front, :], v_sem, 3, 3))
    early[0] = mul3(comb_v[...], data(y))

    def after(k):
        if k != 10:
            return
        moves[0].wait_recv()
        early[1, front, :] = early[1, front, :] + v_far[0]
        moves.append(along(early.at[1, front, :], v_up.at[front, :], v_sem, 4, 1))
        moves[1].wait_recv()
        early[3, back, :] = early[3, back, :] + v_far[1]
        moves.append(along(early.at[3, back, :], v_down.at[back, :], v_sem, 5, 3))

    new = ys[...]
    xg[...] = zs[L:, :] + mm(new, new, over)
    xs[...] = mm(sketch, sketch, over)
    factor_both(xg, xs, u, us, after)
    row = lax.broadcasted_iota(jnp.int32, (K, K), 0)
    lane = lax.broadcasted_iota(jnp.int32, (K, K), 1)
    inner = jnp.where(lane <= row, xs[...], 0.0)
    core[...] = mm(mm(u[...], inner, ((1,), (1,))), inner)
    found = mm(core[...], zs[:L, :], ((1,), (1,)))
    mapping[...] = found
    high = found.astype(jnp.bfloat16)
    rest = found - high.astype(jnp.float32)
    mid = rest.astype(jnp.bfloat16)
    low = (rest - mid.astype(jnp.float32)).astype(jnp.bfloat16)
    table = ts[y]
    comb[:, :256] = mul(high, table) + (mul(mid, table) + mul(low, table))
    comb[:, 256:] = mapping[:, mine]

    rows = x_core.shape[0]
    late = chunks - NY
    half = late // 2

    def spot(place):
        return pl.ds(pl.multiple_of(place * rows, 8), rows)

    far = {}
    for n in [n for i in range(half) for n in (i, half + i)]:
        terms[n] = mul3(comb[...], data(NY + n))
        left = n < half
        far[n] = along(terms.at[n, spot(across), :], far_l.at[n] if left else far_r.at[n - half], far_sem, n, 1 if left else 3)
    to_up, to_down = {}, {}

    def near(n, upward):
        if upward:
            to_up[n] = along(terms.at[n, spot(up), :], near_l.at[n], near_sem, n, 1)
        else:
            to_down[n] = along(terms.at[n, spot(down), :], near_r.at[n], near_sem, late + n, 3)

    for i in range(half):
        near(half + i, True)
        near(i, False)

    for copy in moves[2:]:
        copy.wait_recv()
    found_v[...] = mm(core[...], early[0] + (v_up[...] + v_down[...]))

    def columns(place, start, size):
        return pl.ds(pl.multiple_of(place * CHUNK + start, 128), size)

    wide = CHUNK // 2
    relay_up = along(found_v.at[spot(across), 0:wide], pass_up, x_sem, 0, 1)
    relay_down = along(found_v.at[spot(across), wide:CHUNK], pass_down, x_sem, 1, 3)
    home = [
        along(found_v.at[spot(up), :], x_core.at[:, columns(y, 0, CHUNK)], x_sem, 2, 1),
        along(found_v.at[spot(down), :], x_core.at[:, columns(y, 0, CHUNK)], x_sem, 3, 3),
    ]
    for i in range(half):
        far[i].wait_recv()
        terms[i, spot(up), :] = terms[i, spot(up), :] + far_l[i]
        near(i, True)
        far[half + i].wait_recv()
        terms[half + i, spot(down), :] = terms[half + i, spot(down), :] + far_r[i]
        near(half + i, False)
    relay_up.wait_recv()
    home.append(along(pass_up, x_core.at[:, columns(down, 0, wide)], x_sem, 4, 1))
    relay_down.wait_recv()
    home.append(along(pass_down, x_core.at[:, columns(up, wide, wide)], x_sem, 5, 3))
    x_core[:, columns(y, 0, CHUNK)] = found_v[spot(y), :]

    outer = jnp.where(lane <= row, xg[...], 0.0)
    q_prev[...] = mm(y_prev[...], outer, ((1,), (1,)))
    col = (z * NX + x) * NC + c
    pair = mm(ys[pl.ds(pl.multiple_of(y * 256 + (col // 2) * 8, 8), 8), :], outer, ((1,), (1,)))
    q_new[...] = jnp.where(col % 2 == 0, pair[:4], pair[4:])

    for i in range(half):
        for n in (half + i, i):
            to_up[n].wait_recv()
            to_down[n].wait_recv()
            x_core[:, (NY + n) * CHUNK : (NY + n + 1) * CHUNK] = terms[n, spot(y), :] + (near_l[n] + near_r[n])
    for copy in home:
        copy.wait_recv()
    everything += moves + [relay_up, relay_down] + home + list(far.values()) + list(to_up.values()) + list(to_down.values())
    for copy in everything:
        copy.wait_send()


def hand_over(*refs):
    for source, target in zip(refs[:3], refs[3:]):
        target[...] = source[...]


def whole(slab, omega, y_prev, w_prev, *marks):
    rows, cols = slab.shape
    chunks = cols // CHUNK
    late = chunks - NY
    share = K // NY
    vmem = pl.BlockSpec(memory_space=pltpu.VMEM)
    hbm = pl.BlockSpec(memory_space=pltpu.HBM)
    f32 = jnp.float32
    dma = pltpu.SemaphoreType.DMA

    def buffers(*shapes):
        return [pltpu.VMEM(shape, f32) for shape in shapes]

    found = pl.pallas_call(
        whole_kernel,
        out_shape=(
            jax.ShapeDtypeStruct(y_prev.shape, f32),
            jax.ShapeDtypeStruct((4, K), f32),
            jax.ShapeDtypeStruct((share, cols), f32),
        ),
        in_specs=[hbm] * 8,
        out_specs=[vmem] * 3,
        scratch_shapes=buffers(
            (NC, NY, NX, BLOCK, 128),
            (chunks, rows, CHUNK),
            (chunks, CHUNK, K),
            (chunks, w_prev.shape[0], CHUNK),
            (SUMS, K),
            (rows, K),
            (SUMS, 128),
            (rows, 128),
            (SUMS, 128),
            (rows, 128),
            (2, 3, PART_A, 128),
            (3, PIECE, 128),
            (2, 3, PART_B, 128),
            (7, 8, 128),
            (7, 2 * PART_B, 128),
            (PIECE, 128),
            (2, PART_A, 128),
            (2 * PART_B, 128),
            (K, K),
            (K, K),
            (K, K),
            (K, K),
            (1024, K),
            (SUMS, K),
        )
        + [pltpu.VMEM((NY, L, K), jnp.bfloat16)]
        + buffers(
            (K, 384),
            (K, 384),
            (K, K),
            (K, L),
            (NY, K, CHUNK),
            (2, K // 2, CHUNK),
            (K, CHUNK),
            (K, CHUNK),
            (late, K, CHUNK),
            (late // 2, share, CHUNK),
            (late // 2, share, CHUNK),
            (late, share, CHUNK),
            (late, share, CHUNK),
            (K, CHUNK),
            (share, CHUNK // 2),
            (share, CHUNK // 2),
            y_prev.shape,
        )
        + [pltpu.VMEM((2, 128), jnp.int32)] * 4
        + [
            dma((5,)),
            dma((3, chunks)),
            dma((2, 2)),
            dma((2, 6)),
            dma((2, 3)),
            dma((2, 6)),
            dma((2, 7)),
            dma((2, 7)),
            dma((2, 7)),
            dma((2, 3)),
            dma((2, 12)),
            dma((2, 16)),
            dma((2, 6)),
            dma((2, 6)),
            dma((2, late)),
            dma((2, 2 * late)),
        ],
        compiler_params=pltpu.CompilerParams(collective_id=0, has_side_effects=True, vmem_limit_bytes=67_043_328),
        cost_estimate=pl.CostEstimate(flops=60_000_000_000, bytes_accessed=20_000_000, transcendentals=0),
        name="whole",
    )(slab, omega, y_prev, w_prev, *(mark.reshape(2, 128) for mark in marks))
    return pl.pallas_call(
        hand_over,
        out_shape=[jax.ShapeDtypeStruct(part.shape, f32) for part in found],
        in_specs=[vmem] * 3,
        out_specs=[vmem] * 3,
        name="hand_over",
    )(*found)


def solution(mesh):
    finer = Mesh(mesh.devices.reshape(NZ, NX, NC, NY), ("z", "x", "core", "y"))
    return jax.shard_map(
        whole,
        mesh=finer,
        in_specs=(
            P("y", COL),
            P(COL, None),
            P(ROW_COL, None),
            P("y", COL),
            P(ROW_COL),
            P(ROW_COL),
            P("y"),
            P("y"),
        ),
        out_specs=(P(ROW_COL, None), P(ROW_COL, None), P("y", COL)),
        check_vma=False,
    )
```

```python
import jax
import jax.numpy as jnp
from jax import lax
from jax.experimental import pallas as pl
from jax.experimental.pallas import tpu as pltpu
from jax.sharding import Mesh
from jax.sharding import PartitionSpec as P

L = 512
COL = ("z", "x", "core")
ROW_COL = ("y", "z", "x", "core")
MESH = pl.DeviceIdType.MESH
highest = lax.Precision.HIGHEST
K = 256
BLK = 16
SUP = 64


def mm(a, b, dims=((1,), (0,))):
    return lax.dot_general(a, b, (dims, ((), ())), precision=highest, preferred_element_type=jnp.float32)


def eliminate(panel, k):
    off = k * BLK
    tile = off // 128 * 128
    cols = []
    for j in range(BLK):
        c = off + j
        cols.append([jnp.broadcast_to(panel[h * 8 : h * 8 + 8, c : c + 1], (8, 128)) for h in (0, 1)])
    lane = lax.broadcasted_iota(jnp.int32, (8, K), 1)
    row = lax.broadcasted_iota(jnp.int32, (8, K), 0)
    row1 = lax.broadcasted_iota(jnp.int32, (8, 128), 0)
    inside = (lane >= off) & (lane < off + BLK)
    top = jnp.where(inside, (lane == row + off).astype(jnp.float32), panel[:8])
    bot = jnp.where(inside, (lane == row + off + 8).astype(jnp.float32), panel[8:])
    lane1 = lax.broadcasted_iota(jnp.int32, (8, 128), 1) + tile
    corner = [jnp.zeros((8, 128), jnp.float32), jnp.zeros((8, 128), jnp.float32)]
    scales = []
    for j in range(BLK):
        h, r = divmod(j, 8)
        mine = cols[j]
        pivot = jnp.broadcast_to(mine[h][r : r + 1], (8, 128))
        rs = lax.rsqrt(pivot)
        inv = rs * rs
        scales.append(rs)
        low = mine[1] * inv
        high = None
        if h == 0:
            high = mine[0] * inv
        for m in range(j + 1, BLK):
            hm, rm = divmod(m, 8)
            u = jnp.broadcast_to(mine[hm][rm : rm + 1], (8, 128))
            cols[m][1] = cols[m][1] - low * u
            if hm == 0:
                cols[m][0] = cols[m][0] - high * u
        if h == 0:
            p = jnp.broadcast_to(top[r : r + 1], (8, K))
            hm_ = jnp.where(row1 > r, high, 0.0)
            top = top - jnp.concatenate([hm_, hm_], axis=1) * p
            bot = bot - jnp.concatenate([low, low], axis=1) * p
        else:
            p = jnp.broadcast_to(bot[r : r + 1], (8, K))
            lm_ = jnp.where(row1 > r, low, 0.0)
            bot = bot - jnp.concatenate([lm_, lm_], axis=1) * p
    st = jnp.zeros((8, 128), jnp.float32)
    sb = jnp.zeros((8, 128), jnp.float32)
    for j in range(8):
        st = jnp.where(row1 == j, scales[j], st)
        sb = jnp.where(row1 == j, scales[j + 8], sb)
    top = top * jnp.concatenate([st, st], axis=1)
    bot = bot * jnp.concatenate([sb, sb], axis=1)
    for j in range(BLK):
        for h in (0, 1):
            keep = (lane1 == off + j) & (row1 + 8 * h >= j)
            corner[h] = jnp.where(keep, cols[j][h] * scales[j], corner[h])
    return jnp.concatenate([top, bot], axis=0), jnp.concatenate(corner, axis=0)


def factor_step(w, u, k):
    off = k * BLK
    rows = slice(off, off + BLK)
    panel, corner = eliminate(w[rows, :], k)
    tile = off // 128 * 128
    w[rows, :] = panel
    lane = lax.broadcasted_iota(jnp.int32, (BLK, K), 1)
    upper = jnp.where(lane >= off + BLK, panel, 0.0)
    u[rows, :] = upper
    sup_end = (off // SUP + 1) * SUP
    if off + BLK < sup_end:
        turned = panel[:, tile : tile + 128].T
        left = turned[off + BLK - tile : sup_end - tile]
        rest = slice(off + BLK, sup_end)
        lane2 = lax.broadcasted_iota(jnp.int32, (sup_end - off - BLK, K), 1)
        old = jnp.where((lane2 >= off) & (lane2 < off + BLK), 0.0, w[rest, :])
        w[rest, :] = old - mm(left, panel)
    elif sup_end < K:
        start = sup_end - SUP
        block = w[start:sup_end, :]
        t0 = sup_end // 128 * 128
        turned = block[:, t0:].T
        left = turned[sup_end - t0 :]
        rest = slice(sup_end, K)
        lane2 = lax.broadcasted_iota(jnp.int32, (K - sup_end, K), 1)
        old = jnp.where((lane2 >= start) & (lane2 < sup_end), 0.0, w[rest, :])
        lane3 = lax.broadcasted_iota(jnp.int32, (SUP, K), 1)
        row3 = lax.broadcasted_iota(jnp.int32, (SUP, K), 0) + start
        block = jnp.where((lane3 < sup_end) & (lane3 > row3), 0.0, block)
        w[rest, :] = old - mm(left, block)
    return corner


def factor_both(wg, ws, ug, us, after):
    for k in range(K // BLK):
        cg = factor_step(wg, ug, k)
        factor_step(ws, us, k)
        off = k * BLK
        tile = off // 128 * 128
        rows = slice(off, off + BLK)
        turned = cg.T[off - tile : off - tile + BLK]
        ug[rows, off:off + BLK] = turned
        after(k)


NZ, NX, NC, NY = 8, 4, 2, 4
CHUNK = 512
SUMS = L + K
PART_A = SUMS // 2 // NY
PART_B = PART_A // NX
PIECE = K // NX
BLOCK = PIECE + 2 * PART_B + 8


def split(v):
    high = v.astype(jnp.bfloat16)
    return high, (v - high.astype(jnp.float32)).astype(jnp.bfloat16)


def mul(a, b, dims=((1,), (0,))):
    return lax.dot_general(a, b, (dims, ((), ())), preferred_element_type=jnp.float32)


def mul3(a, b, dims=((1,), (0,))):
    ah, al = split(a)
    bh, bl = split(b)
    return mul(ah, bh, dims) + (mul(ah, bl, dims) + mul(al, bh, dims))


def signed_sum(table, v):
    high = v.astype(jnp.bfloat16)
    rest = v - high.astype(jnp.float32)
    mid = rest.astype(jnp.bfloat16)
    low = (rest - mid.astype(jnp.float32)).astype(jnp.bfloat16)
    return mul(table, high) + (mul(table, mid) + mul(table, low))


def table_of(bucket, sign):
    level = lax.broadcasted_iota(jnp.int32, (L, bucket.shape[1]), 0).astype(jnp.float32)
    return jnp.where(level == bucket, 2.0 * sign - 1.0, 0.0).astype(jnp.bfloat16)


def whole_kernel(slab, omega, y_prev, w_prev, prev_bucket, prev_sign, slab_bucket, slab_sign, q_prev, q_new, x_core,
                 out, slab_v, omega_v, w_v, stack, part, got_sums, got_part, chip_sums, chip_part, got_a, got_b, got_s,
                 got_c, got_z, mid_p, mid_a, mid_s, xg, xs, u, us, ys, zs, ts, comb, comb_v, core, mapping,
                 early, v_far, v_up, v_down, terms, far_l, far_r, near_l, near_r, found_v, pass_up, pass_down,
                 load_sem, swap_sem, a_sem, b_sem, s_sem, c_sem, z_sem, d_sem, e_sem, f_sem, g_sem, v_sem, x_sem, far_sem, near_sem):
    z, x, c, y = (lax.axis_index(name) for name in ("z", "x", "core", "y"))

    def at(dz=0, dx=0, dc=0, dy=0):
        return {"z": (z + dz) % NZ, "x": (x + dx) % NX, "core": (c + dc) % NC, "y": (y + dy) % NY}

    def send(src, dst, sems, i, where):
        copy = pltpu.make_async_remote_copy(
            src_ref=src, dst_ref=dst, send_sem=sems.at[0, i], recv_sem=sems.at[1, i], device_id=where, device_id_type=MESH
        )
        copy.start()
        return copy

    barrier = pltpu.get_barrier_semaphore()
    peers = [at(dz=d) for d in range(1, NZ)]
    peers += [at(dy=d) for d in range(1, NY)] + [at(dx=d) for d in range(1, NX)] + [at(dc=1)]
    for peer in peers:
        pl.semaphore_signal(barrier, inc=1, device_id=peer, device_id_type=MESH)

    chunks = slab_v.shape[0]
    loads = []
    for i in range(chunks):
        loads.append(pltpu.make_async_copy(slab.at[:, pl.ds(i * CHUNK, CHUNK)], slab_v.at[i], load_sem.at[0, i]))
        loads.append(pltpu.make_async_copy(omega.at[pl.ds(i * CHUNK, CHUNK), :], omega_v.at[i], load_sem.at[1, i]))
    for load in loads:
        load.start()
    for i in range(chunks):
        pltpu.make_async_copy(w_prev.at[:, pl.ds(i * CHUNK, CHUNK)], w_v.at[i], load_sem.at[2, i]).start()

    def real(ref):
        return ref[...].astype(jnp.float32)

    bucket, sign = real(prev_bucket), real(prev_sign)
    table = jnp.concatenate([table_of(bucket[h : h + 1], sign[h : h + 1]) for h in (0, 1)], axis=1)
    own = y_prev[...]
    stack[:L, :] = signed_sum(table, own)
    stack[L:, :] = mm(own, own, ((0,), (0,)))
    out[c, y, x, PIECE + 2 * PART_B :, :] = jnp.concatenate([real(slab_bucket), real(slab_sign), jnp.zeros((4, 128), jnp.float32)])
    part[...] = jnp.zeros_like(part)

    def multiply(i):
        pltpu.make_async_copy(slab.at[:, pl.ds(0, CHUNK)], slab_v.at[i], load_sem.at[0, i]).wait()
        pltpu.make_async_copy(omega.at[pl.ds(0, CHUNK), :], omega_v.at[i], load_sem.at[1, i]).wait()
        part[...] += mul3(slab_v[i], omega_v[i])

    pl.loop(0, chunks)(multiply)
    pl.semaphore_wait(barrier, len(peers))

    ours = pl.ds(pl.multiple_of(c * 128, 128), 128)
    theirs = pl.ds(pl.multiple_of((1 - c) * 128, 128), 128)
    swap_sums = send(stack.at[:, theirs], got_sums, swap_sem, 0, at(dc=1))
    swap_part = send(part.at[:, theirs], got_part, swap_sem, 1, at(dc=1))

    def share(half, where):
        place = where["x"] if half else where["y"]
        return pl.ds(pl.multiple_of(half * (SUMS // 2) + place * PART_A, 8), PART_A)

    swap_sums.wait_recv()
    chip_sums[...] = stack[:, ours] + got_sums[...]
    sent_a = []
    for d in (2, 1, 3):
        for half in (0, 1):
            where = at(dx=d) if half else at(dy=d)
            sent_a.append(send(chip_sums.at[share(half, where), :], got_a.at[half, d - 1], a_sem, 2 * (d - 1) + half, where))

    swap_part.wait_recv()
    chip_part[...] = part[:, ours] + got_part[...]
    sent_b = []
    for d in (2, 1, 3):
        where = at(dx=d)
        piece = chip_part.at[pl.ds(pl.multiple_of(where["x"] * PIECE, 8), PIECE), :]
        sent_b.append(send(piece, got_b.at[d - 1], b_sem, d - 1, where))

    for copy in sent_a:
        copy.wait_recv()
    for half in (0, 1):
        total = chip_sums[share(half, at()), :]
        for d in range(1, 4):
            total = total + got_a[half, d - 1]
        mid_a[half] = total
    sent_s = []
    for d in range(1, NX):
        for half in (0, 1):
            where = at(dy=d) if half else at(dx=d)
            place = where["y"] if half else where["x"]
            piece = mid_a.at[half, pl.ds(pl.multiple_of(place * PART_B, 8), PART_B), :]
            sent_s.append(send(piece, got_s.at[half, d - 1], s_sem, 2 * (d - 1) + half, where))

    for copy in sent_b:
        copy.wait_recv()
    total = chip_part[pl.ds(pl.multiple_of(x * PIECE, 8), PIECE), :]
    for d in range(1, NX):
        total = total + got_b[d - 1]
    mid_p[...] = total
    sent_c = []
    for d in range(1, NZ):
        where = at(dz=d)
        piece = mid_p.at[pl.ds(pl.multiple_of(where["z"] * 8, 8), 8), :]
        sent_c.append(send(piece, got_c.at[d - 1], c_sem, d - 1, where))

    for copy in sent_s:
        copy.wait_recv()
    for half in (0, 1):
        total = mid_a[half, pl.ds(pl.multiple_of((y if half else x) * PART_B, 8), PART_B), :]
        for d in range(1, NX):
            total = total + got_s[half, d - 1]
        mid_s[half * PART_B : half * PART_B + PART_B, :] = total
    sent_z = [send(mid_s, got_z.at[d - 1], z_sem, d - 1, at(dz=d)) for d in range(1, NZ)]

    for copy in sent_c:
        copy.wait_recv()
    total = mid_p[pl.ds(pl.multiple_of(z * 8, 8), 8), :]
    for d in range(1, NZ):
        total = total + got_c[d - 1]
    tile = pl.ds(pl.multiple_of(z * 8, 8), 8)
    out[c, y, x, tile, :] = total
    sent_d = [send(out.at[c, y, x, tile, :], out.at[c, y, x, tile, :], d_sem, d - 1, at(dz=d)) for d in range(1, NZ)]

    for copy in sent_z:
        copy.wait_recv()
    total = mid_s[...]
    for d in range(1, NZ):
        total = total + got_z[d - 1]
    out[c, y, x, PIECE : PIECE + 2 * PART_B, :] = total
    for copy in sent_d:
        copy.wait_recv()

    def first(d):
        return at(dx=d * (1 - c), dy=d * c)

    def second(d):
        return at(dx=d * c, dy=d * (1 - c))

    def gathered(n, d):
        return out.at[c, (y + (4 - n) * c + (4 - d) * (1 - c)) % NY, (x + (4 - n) * (1 - c) + (4 - d) * c) % NX]

    def swap(n, d):
        block = gathered(n, d)
        return send(block, block, g_sem, 4 * n + d, at(dc=1))

    def both_ways(n):
        block = gathered(n, 0)
        return [send(block, block, f_sem, 3 * n + d - 1, second(d)) for d in (1, 3)]

    own_block = gathered(0, 0)
    sent_e = [send(own_block, own_block, e_sem, d - 1, first(d)) for d in range(1, 4)]
    sent_f = {0: both_ways(0)}
    sent_g = [swap(0, 0)]
    for n in (1, 3, 2):
        sent_e[n - 1].wait_recv()
        sent_f[n] = both_ways(n)
        sent_g.append(swap(n, 0))
    passed = []
    for n in (0, 1, 3, 2):
        for d in (1, 3):
            sent_f[n][d // 2].wait_recv()
            block = gathered(n, d)
            if d == (1, 3)[n % 2]:
                passed.append((n, send(block, block, f_sem, 3 * n + 1, second(d))))
            sent_g.append(swap(n, d))
    for n, copy in passed:
        copy.wait_recv()
        sent_g.append(swap(n, 2))
    sent_f = [copy for n in range(4) for copy in sent_f[n]] + [copy for _, copy in passed]
    for copy in sent_g:
        copy.wait_recv()
    everything = [swap_sums, swap_part] + sent_a + sent_b + sent_s + sent_c + sent_z + sent_d + sent_e + sent_f + sent_g

    for cc in range(NC):
        lanes = slice(128 * cc, 128 * cc + 128)
        for yy in range(NY):
            for xx in range(NX):
                ys[pl.ds(256 * yy + PIECE * xx, PIECE), lanes] = out[cc, yy, xx, :PIECE, :]
                for half in (0, 1):
                    start = half * (SUMS // 2) + (PART_A * xx + PART_B * yy if half else PART_A * yy + PART_B * xx)
                    zs[pl.ds(start, PART_B), lanes] = out[cc, yy, xx, PIECE + half * PART_B : PIECE + half * PART_B + PART_B, :]
    for yy in range(NY):
        marks = out[0, yy, 0, PIECE + 2 * PART_B :, :]
        for h in (0, 1):
            ts[yy, :, 128 * h : 128 * h + 128] = table_of(marks[h : h + 1], marks[h + 2 : h + 3])
    new = ys[...]
    xg[...] = zs[L:, :] + mm(new, new, ((0,), (0,)))
    sketch = zs[:L, :]
    for yy in range(NY):
        sketch = sketch + signed_sum(ts[yy], ys[256 * yy : 256 * yy + 256, :])
    zs[:L, :] = sketch

    up, across, down = (y + 1) % NY, (y + 2) % NY, (y + 3) % NY
    mine = pl.ds(pl.multiple_of(y * 128, 128), 128)
    for i in range(chunks):
        pltpu.make_async_copy(w_prev.at[:, pl.ds(0, CHUNK)], w_v.at[i], load_sem.at[2, i]).wait()
    high = sketch.astype(jnp.bfloat16)
    rest = sketch - high.astype(jnp.float32)
    mid = rest.astype(jnp.bfloat16)
    low = (rest - mid.astype(jnp.float32)).astype(jnp.bfloat16)
    table = ts[y]
    over = ((0,), (0,))
    comb_v[:, :256] = mul(high, table, over) + (mul(mid, table, over) + mul(low, table, over))
    comb_v[:, 256:] = zs[mine, :].T

    def data(n):
        return jnp.concatenate([slab_v[n], w_v[n]], axis=0)

    def along(src, dst, sems, i, peer):
        return send(src, dst, sems, i, at(dy=peer))

    front, back = slice(0, K // 2), slice(K // 2, K)
    early[2] = mul3(comb_v[...], data(across))
    moves = [
        along(early.at[2, front, :], v_far.at[0], v_sem, 0, 1),
        along(early.at[2, back, :], v_far.at[1], v_sem, 1, 3),
    ]
    early[1] = mul3(comb_v[...], data(up))
    moves.append(along(early.at[1, back, :], v_up.at[back, :], v_sem, 2, 1))
    early[3] = mul3(comb_v[...], data(down))
    moves.append(along(early.at[3, front, :], v_down.at[front, :], v_sem, 3, 3))
    early[0] = mul3(comb_v[...], data(y))

    def after(k):
        if k != 10:
            return
        moves[0].wait_recv()
        early[1, front, :] = early[1, front, :] + v_far[0]
        moves.append(along(early.at[1, front, :], v_up.at[front, :], v_sem, 4, 1))
        moves[1].wait_recv()
        early[3, back, :] = early[3, back, :] + v_far[1]
        moves.append(along(early.at[3, back, :], v_down.at[back, :], v_sem, 5, 3))

    xs[...] = mm(sketch, sketch, over)
    factor_both(xg, xs, u, us, after)
    row = lax.broadcasted_iota(jnp.int32, (K, K), 0)
    lane = lax.broadcasted_iota(jnp.int32, (K, K), 1)
    inner = jnp.where(lane <= row, xs[...], 0.0)
    core[...] = mm(mm(u[...], inner, ((1,), (1,))), inner)
    found = mm(core[...], zs[:L, :], ((1,), (1,)))
    mapping[...] = found
    high = found.astype(jnp.bfloat16)
    rest = found - high.astype(jnp.float32)
    mid = rest.astype(jnp.bfloat16)
    low = (rest - mid.astype(jnp.float32)).astype(jnp.bfloat16)
    table = ts[y]
    comb[:, :256] = mul(high, table) + (mul(mid, table) + mul(low, table))
    comb[:, 256:] = mapping[:, mine]

    rows = x_core.shape[0]
    late = chunks - NY
    half = late // 2

    def spot(place):
        return pl.ds(pl.multiple_of(place * rows, 8), rows)

    far = {}
    for n in [n for i in range(half) for n in (i, half + i)]:
        terms[n] = mul3(comb[...], data(NY + n))
        left = n < half
        far[n] = along(terms.at[n, spot(across), :], far_l.at[n] if left else far_r.at[n - half], far_sem, n, 1 if left else 3)
    to_up, to_down = {}, {}

    def near(n, upward):
        if upward:
            to_up[n] = along(terms.at[n, spot(up), :], near_l.at[n], near_sem, n, 1)
        else:
            to_down[n] = along(terms.at[n, spot(down), :], near_r.at[n], near_sem, late + n, 3)

    for i in range(half):
        near(half + i, True)
        near(i, False)

    for copy in moves[2:]:
        copy.wait_recv()
    found_v[...] = mm(core[...], early[0] + (v_up[...] + v_down[...]))

    def columns(place, start, size):
        return pl.ds(pl.multiple_of(place * CHUNK + start, 128), size)

    wide = CHUNK // 2
    relay_up = along(found_v.at[spot(across), 0:wide], pass_up, x_sem, 0, 1)
    relay_down = along(found_v.at[spot(across), wide:CHUNK], pass_down, x_sem, 1, 3)
    home = [
        along(found_v.at[spot(up), :], x_core.at[:, columns(y, 0, CHUNK)], x_sem, 2, 1),
        along(found_v.at[spot(down), :], x_core.at[:, columns(y, 0, CHUNK)], x_sem, 3, 3),
    ]
    for i in range(half):
        far[i].wait_recv()
        terms[i, spot(up), :] = terms[i, spot(up), :] + far_l[i]
        near(i, True)
        far[half + i].wait_recv()
        terms[half + i, spot(down), :] = terms[half + i, spot(down), :] + far_r[i]
        near(half + i, False)
    relay_up.wait_recv()
    home.append(along(pass_up, x_core.at[:, columns(down, 0, wide)], x_sem, 4, 1))
    relay_down.wait_recv()
    home.append(along(pass_down, x_core.at[:, columns(up, wide, wide)], x_sem, 5, 3))
    x_core[:, columns(y, 0, CHUNK)] = found_v[spot(y), :]

    outer = jnp.where(lane <= row, xg[...], 0.0)
    q_prev[...] = mm(y_prev[...], outer, ((1,), (1,)))
    col = (z * NX + x) * NC + c
    pair = mm(ys[pl.ds(pl.multiple_of(y * 256 + (col // 2) * 8, 8), 8), :], outer, ((1,), (1,)))
    q_new[...] = jnp.where(col % 2 == 0, pair[:4], pair[4:])

    for i in range(half):
        for n in (half + i, i):
            to_up[n].wait_recv()
            to_down[n].wait_recv()
            x_core[:, (NY + n) * CHUNK : (NY + n + 1) * CHUNK] = terms[n, spot(y), :] + (near_l[n] + near_r[n])
    for copy in home:
        copy.wait_recv()
    everything += moves + [relay_up, relay_down] + home + list(far.values()) + list(to_up.values()) + list(to_down.values())
    for copy in everything:
        copy.wait_send()


def hand_over(*refs):
    for source, target in zip(refs[:3], refs[3:]):
        target[...] = source[...]


def whole(slab, omega, y_prev, w_prev, *marks):
    rows, cols = slab.shape
    chunks = cols // CHUNK
    late = chunks - NY
    share = K // NY
    vmem = pl.BlockSpec(memory_space=pltpu.VMEM)
    hbm = pl.BlockSpec(memory_space=pltpu.HBM)
    f32 = jnp.float32
    dma = pltpu.SemaphoreType.DMA

    def buffers(*shapes):
        return [pltpu.VMEM(shape, f32) for shape in shapes]

    found = pl.pallas_call(
        whole_kernel,
        out_shape=(
            jax.ShapeDtypeStruct(y_prev.shape, f32),
            jax.ShapeDtypeStruct((4, K), f32),
            jax.ShapeDtypeStruct((share, cols), f32),
        ),
        in_specs=[hbm, hbm, vmem, hbm] + [vmem] * 4,
        out_specs=[vmem] * 3,
        scratch_shapes=buffers(
            (NC, NY, NX, BLOCK, 128),
            (chunks, rows, CHUNK),
            (chunks, CHUNK, K),
            (chunks, w_prev.shape[0], CHUNK),
            (SUMS, K),
            (rows, K),
            (SUMS, 128),
            (rows, 128),
            (SUMS, 128),
            (rows, 128),
            (2, 3, PART_A, 128),
            (3, PIECE, 128),
            (2, 3, PART_B, 128),
            (7, 8, 128),
            (7, 2 * PART_B, 128),
            (PIECE, 128),
            (2, PART_A, 128),
            (2 * PART_B, 128),
            (K, K),
            (K, K),
            (K, K),
            (K, K),
            (1024, K),
            (SUMS, K),
        )
        + [pltpu.VMEM((NY, L, K), jnp.bfloat16)]
        + buffers(
            (K, 384),
            (K, 384),
            (K, K),
            (K, L),
            (NY, K, CHUNK),
            (2, K // 2, CHUNK),
            (K, CHUNK),
            (K, CHUNK),
            (late, K, CHUNK),
            (late // 2, share, CHUNK),
            (late // 2, share, CHUNK),
            (late, share, CHUNK),
            (late, share, CHUNK),
            (K, CHUNK),
            (share, CHUNK // 2),
            (share, CHUNK // 2),
        )
        + [
            dma((3, chunks)),
            dma((2, 2)),
            dma((2, 6)),
            dma((2, 3)),
            dma((2, 6)),
            dma((2, 7)),
            dma((2, 7)),
            dma((2, 7)),
            dma((2, 3)),
            dma((2, 12)),
            dma((2, 16)),
            dma((2, 6)),
            dma((2, 6)),
            dma((2, late)),
            dma((2, 2 * late)),
        ],
        compiler_params=pltpu.CompilerParams(collective_id=0, has_side_effects=True, vmem_limit_bytes=67_043_328),
        cost_estimate=pl.CostEstimate(flops=60_000_000_000, bytes_accessed=20_000_000, transcendentals=0),
        name="whole",
    )(slab, omega, y_prev, w_prev, *(mark.reshape(2, 128) for mark in marks))
    return pl.pallas_call(
        hand_over,
        out_shape=[jax.ShapeDtypeStruct(part.shape, f32) for part in found],
        in_specs=[vmem] * 3,
        out_specs=[vmem] * 3,
        name="hand_over",
    )(*found)


def solution(mesh):
    finer = Mesh(mesh.devices.reshape(NZ, NX, NC, NY), ("z", "x", "core", "y"))
    return jax.shard_map(
        whole,
        mesh=finer,
        in_specs=(
            P("y", COL),
            P(COL, None),
            P(ROW_COL, None),
            P("y", COL),
            P(ROW_COL),
            P(ROW_COL),
            P("y"),
            P("y"),
        ),
        out_specs=(P(ROW_COL, None), P(ROW_COL, None), P("y", COL)),
        check_vma=False,
    )
```
